32 devices in a mesh: replica: 8 (over z, y), shard: 4 (over x, core).
Axes of the slice: x: 2, y: 2, z: 4, core: 2. Of those that a mesh axis runs over, the one named last changes fastest.
Arguments:
- outer_params: float32 [512, 4096], P('shard'), may hold values from -6 to 6, as said below
- local_params: bfloat16 [8, 512, 4096], P('replica', 'shard'), may hold values from -70 to 70
- momentum: float32 [512, 4096], P('shard'), may hold values from -6 to 6
Outputs:
- params_next: float32 [512, 4096], P('shard')
- momentum_next: float32 [512, 4096], P('shard')
- block_scales: float32 [32, 512], P(None, 'shard')
The draws below stay inside these ranges and needn't reach their ends.
Inputs may be any that keep to these rules, and one draw needn't show every extreme that they name: `outer_params`: outer parameters of order one.
All inputs are finite; a program needn't handle non-finite values.
Results may differ from the reference program's by a relative error of at most 0.005.
Values may be sent and summed in bfloat16 or wider, within the bound.
A program may use at most 64 MiB of HBM per device.

```python
import math
import jax
import jax.numpy as jnp
from jax import lax

D = 4096
BLOCK = 128
ROWS = 512
WORKERS = 8


def draw_fields(key):
    base_key = jax.random.fold_in(key, 71)
    outer_key = jax.random.fold_in(base_key, 1)
    column_key = jax.random.fold_in(base_key, 2)
    common_key = jax.random.fold_in(base_key, 3)
    noise_key = jax.random.fold_in(base_key, 4)
    level_key = jax.random.fold_in(base_key, 5)
    group_rows = 32
    group_count = (ROWS + group_rows - 1) // group_rows
    raw_levels = jax.random.uniform(level_key, (group_count,), jnp.float32, 0.0, 1.0)
    unit_levels = raw_levels - jnp.max(raw_levels) + 1.0
    row_group = jnp.arange(ROWS, dtype=jnp.int32) // group_rows
    row_scale = 10.0 ** unit_levels[row_group]
    common_part = jnp.clip(jax.random.normal(common_key, (ROWS, D), jnp.float32), -4.0, 4.0)
    noise_part = jnp.clip(jax.random.normal(noise_key, (WORKERS, ROWS, D), jnp.float32), -4.0, 4.0)
    column_scale = jnp.exp(jax.random.uniform(column_key, (D,), jnp.float32, 0.0, math.log(10.0)))
    outer_values = jnp.clip(jax.random.normal(outer_key, (ROWS, D), jnp.float32), -6.0, 6.0)
    deltas = 0.05 * row_scale[:, None] * column_scale[None, :] * (common_part[None] + noise_part)
    return (outer_values, deltas)


def draw_outer_params(key, part):
    outer_values, deltas = draw_fields(key)
    return outer_values


def draw_local_params(key, part):
    outer_values, deltas = draw_fields(key)
    return (outer_values[None] - deltas).astype(jnp.bfloat16)


def block_scale(stream_key, extent, pieces, low, high):
    level = 1.0
    for axis_at, shards_of in pieces:
        draws = jax.random.uniform(jax.random.fold_in(jax.random.fold_in(stream_key, 6), axis_at), (shards_of,), jnp.float32, low / len(pieces), high / len(pieces))
        level = level * jnp.repeat(jnp.exp(draws), extent[axis_at] // shards_of).reshape((-1,) + (1,) * (len(extent) - 1 - axis_at))
    return level


def scatter_about(stream_key, dims, scale, most, pieces=(), kind=jnp.bfloat16):
    values = jax.random.normal(stream_key, dims, jnp.float32) * scale
    if len(pieces) > 0:
        values = block_scale(stream_key, dims, pieces, -0.22, 0.18) * values
    return jnp.clip(values, min=-most, max=most).astype(kind)


def setup_inputs(seed: int = 0) -> dict:
    seeds = jax.random.split(jax.random.key(seed), 4)
    outer_params = draw_outer_params(jax.random.fold_in(seeds[3], 71), 0)
    local_params = draw_local_params(jax.random.fold_in(seeds[3], 71), 0)
    momentum = scatter_about(seeds[2], (ROWS, D), 1.0, 6.0, ((0, 4),), jnp.float32)
    return {"outer_params": outer_params, "local_params": local_params, "momentum": momentum}


epsilon = 1e-06
clip_level = 0.5
outer_rate = 0.7
outer_decay = 0.9
grid_levels = 7.0

def smooth_step(values):
    return values - jnp.sin(2.0 * math.pi * values) / (2.0 * math.pi)

def smooth_round(values):
    return smooth_step(smooth_step(values))

def block_max(values):
    return lax.optimization_barrier(jnp.max(jnp.abs(values).reshape(values.shape[0], D // BLOCK, BLOCK), axis=2))

def reference(outer_params, local_params, momentum):

    def worker_max(running, worker_local):
        deltas = outer_params - worker_local.astype(jnp.float32)
        return (jnp.maximum(running, block_max(deltas)), None)
    absmax, _ = lax.scan(worker_max, jnp.zeros((ROWS, D // BLOCK), jnp.float32), local_params)
    spread_scale = jnp.repeat(absmax + epsilon, BLOCK, axis=1)

    def worker_sum(running, worker_local):
        deltas = outer_params - worker_local.astype(jnp.float32)
        encoded = smooth_round(grid_levels * deltas / spread_scale).astype(jnp.bfloat16)
        return (running + spread_scale * encoded.astype(jnp.float32) / grid_levels, None)
    summed_rows, _ = lax.scan(worker_sum, jnp.zeros((ROWS, D), jnp.float32), local_params)
    gradient = summed_rows / WORKERS
    root_mean = jnp.sqrt(jnp.mean(gradient * gradient) + epsilon)
    factor = jnp.minimum(1.0, clip_level / root_mean)
    clipped = factor * gradient
    momentum_next = outer_decay * momentum + clipped
    params_next = outer_params - outer_rate * (clipped + outer_decay * momentum_next)
    return (params_next, momentum_next, absmax.T)
```

```python
import functools

import jax
import jax.numpy as jnp
from jax import lax
from jax.experimental import pallas as pl
from jax.experimental.pallas import tpu as pltpu
from jax.sharding import PartitionSpec as P

BLOCK = 128
MESH = pl.DeviceIdType.MESH

epsilon = 1e-06
clip_level = 0.5
outer_rate = 0.7
outer_decay = 0.9
grid_levels = 7.0

SMOOTH = (6.57973588, -12.98785441, 12.20756634, -6.687892761, 2.368806331, -0.5120006377)
SHIFT = 1.5 * 2.0**23
SQUARE = 4
CODE_RANGE = 112.0
PARTS = 4


def smooth_rest(rest):
    square = rest * rest
    value = SMOOTH[-1]
    for coefficient in SMOOTH[-2::-1]:
        value = value * square + coefficient
    return rest * square * value


def column_of(row):
    return jnp.broadcast_to(row, (BLOCK, row.shape[1])).T


def encode(deltas, inverse):
    values = deltas * inverse
    nearest = (values + SHIFT) - SHIFT
    rest = smooth_rest(smooth_rest(values - nearest))
    return (nearest + rest).astype(jnp.bfloat16).astype(jnp.float32)


def pack(total, most):
    return jnp.exp2(total * (CODE_RANGE / most)).astype(jnp.bfloat16)


def unpack(code, most):
    return jnp.log2(code.astype(jnp.float32)) * (most / CODE_RANGE)


def exchange_kernel(
    workers, shards, entry_count,
    outer_hbm, local_hbm, momentum_hbm, gradient_out, momentum_out, max_out, factor_out,
    outer_v, local_v, raw, local_max, max_slots, inverse, spread, own_sum, staged, arrived, gathered, squares, shard_squares,
    load_sem, raw_send, raw_recv, max_send, max_recv, top_send, top_recv, sum_send, sum_recv,
    sq_send, sq_recv, ss_send, ss_recv, gat_send, gat_recv, fwd_send, fwd_recv, momentum_sem,
):
    me = lax.axis_index("replica")
    my_shard = lax.axis_index("shard")
    rows, cols = outer_v.shape
    quarter = cols // SQUARE
    width = cols // workers
    blocks_each = width // BLOCK
    quarter_blocks = quarter // BLOCK
    squares_count = workers // SQUARE
    parts = gathered.shape[0]
    part_rows = rows // parts
    most_square = grid_levels * SQUARE
    most_all = grid_levels * workers

    position = lax.rem(me, SQUARE)
    my_square = me // SQUARE
    low = lax.rem(me, 2)
    high = me // 2
    pairs = workers // 2
    flipped = position + 1 - 2 * low
    across = lax.rem(position + 2, SQUARE)
    diagonal = lax.rem(flipped + 2, SQUARE)
    mates = (diagonal, flipped, across)
    partner = me + 1 - 2 * low

    def peer(step):
        return lax.rem(me + step, workers)

    def span(start, size):
        return pl.ds(pl.multiple_of(start, BLOCK), size)

    def loads(i):
        part = pl.ds(i * quarter, quarter)
        return (
            pltpu.make_async_copy(outer_hbm.at[:, part], outer_v.at[:, part], load_sem.at[0, i]),
            pltpu.make_async_copy(local_hbm.at[0, :, part], local_v.at[:, part], load_sem.at[1, i]),
        )

    for i in range(SQUARE):
        for copy in loads(i):
            copy.start()
    momentum_copy = pltpu.make_async_copy(momentum_hbm, momentum_out, momentum_sem)

    barrier = pltpu.get_barrier_semaphore()

    @pl.loop(1, workers)
    def _(step):
        pl.semaphore_signal(barrier, inc=1, device_id={"replica": peer(step)}, device_id_type=MESH)

    @pl.loop(1, shards)
    def _(step):
        pl.semaphore_signal(
            barrier, inc=1, device_id={"shard": lax.rem(my_shard + step, shards)}, device_id_type=MESH
        )

    def rows_of(part):
        return pl.ds(pl.multiple_of(part * part_rows, part_rows), part_rows)

    def raw_copy(part, mate):
        return pltpu.make_async_remote_copy(
            src_ref=local_v.at[rows_of(part), span(mates[mate] * quarter, quarter)],
            dst_ref=raw.at[mate, rows_of(part), :],
            send_sem=raw_send.at[part, mate], recv_sem=raw_recv.at[part, mate],
            device_id={"replica": my_square * SQUARE + mates[mate]}, device_id_type=MESH,
        )

    def max_copy(step):
        target = lax.rem(peer(step), SQUARE)
        return pltpu.make_async_remote_copy(
            src_ref=local_max.at[pl.ds(pl.multiple_of(target * quarter_blocks, quarter_blocks), quarter_blocks)],
            dst_ref=max_slots.at[me],
            send_sem=max_send.at[step], recv_sem=max_recv.at[step],
            device_id={"replica": peer(step)}, device_id_type=MESH,
        )

    together = min(4, quarter_blocks)
    for i in range(SQUARE):
        for copy in loads(i):
            copy.wait()

        @pl.loop(0, quarter_blocks // together)
        def _(group):
            for j in range(together):
                block = i * quarter_blocks + group * together + j
                at = span(block * BLOCK, BLOCK)
                deltas = outer_v[:, at] - local_v[:, at].astype(jnp.float32)
                local_max[pl.ds(block, 1), :] = jnp.max(jnp.abs(deltas).T, axis=0, keepdims=True)

    mine = pl.ds(pl.multiple_of(position * quarter_blocks, quarter_blocks), quarter_blocks)
    max_slots[me] = local_max[mine]
    pl.semaphore_wait(barrier, workers + shards - 2)

    @pl.loop(1, workers)
    def _(step):
        max_copy(step).start()

    @pl.loop(0, parts)
    def _(part):
        for mate in range(3):
            raw_copy(part, mate).start()

    momentum_copy.start()

    @pl.loop(1, workers)
    def _(step):
        max_copy(step).wait()

    absmax = max_slots[0]
    for w in range(1, workers):
        absmax = jnp.maximum(absmax, max_slots[w])
    max_out[mine] = absmax
    scale = absmax + epsilon

    def top_copy(mate):
        return pltpu.make_async_remote_copy(
            src_ref=max_out.at[mine], dst_ref=max_out.at[mine],
            send_sem=top_send.at[mate], recv_sem=top_recv.at[mate],
            device_id={"replica": my_square * SQUARE + mates[mate]}, device_id_type=MESH,
        )

    quotient = grid_levels / scale
    for block in range(quarter_blocks):
        inverse[:, block * BLOCK : (block + 1) * BLOCK] = column_of(quotient[block : block + 1, :])
    for mate in range(3):
        top_copy(mate).start()

    def spread_column(block):
        row = (max_out[pl.ds(block, 1), :] + epsilon) * (1.0 / (grid_levels * workers))
        spread[:, span(block * BLOCK, BLOCK)] = column_of(row)

    def place(worker):
        return lax.rem(worker, SQUARE) * quarter + (worker // SQUARE) * width

    @pl.loop(0, quarter_blocks)
    def _(block):
        spread_column(position * quarter_blocks + block)

    def square_of(turn):
        return lax.rem(my_square + turn, squares_count)

    def sum_copy(part, turn):
        return pltpu.make_async_remote_copy(
            src_ref=staged.at[square_of(turn), rows_of(part)], dst_ref=arrived.at[my_square, rows_of(part)],
            send_sem=sum_send.at[part, turn], recv_sem=sum_recv.at[part, turn],
            device_id={"replica": square_of(turn) * SQUARE + position}, device_id_type=MESH,
        )

    def square_sum(part, block):
        at_rows = rows_of(part)
        at = span(position * quarter + block * BLOCK, BLOCK)
        here = span(block * BLOCK, BLOCK)
        outer = outer_v[at_rows, at]
        inv = inverse[at_rows, here]
        total = encode(outer - local_v[at_rows, at].astype(jnp.float32), inv)
        for mate in range(3):
            total = total + encode(outer - raw[mate, at_rows, here].astype(jnp.float32), inv)
        return total

    def encode_part(part):
        for mate in range(3):
            raw_copy(part, mate).wait_recv()

        @pl.loop(1, squares_count)
        def _(turn):
            target = square_of(turn)
            for i in range(blocks_each):
                staged[target, rows_of(part), i * BLOCK : (i + 1) * BLOCK] = pack(
                    square_sum(part, target * blocks_each + i), most_square
                )

        for i in range(blocks_each):
            own_sum[rows_of(part), i * BLOCK : (i + 1) * BLOCK] = square_sum(part, my_square * blocks_each + i)

        @pl.loop(1, squares_count)
        def _(turn):
            sum_copy(part, turn).start()

    def gat_copy(part, step):
        return pltpu.make_async_remote_copy(
            src_ref=gathered.at[part, me], dst_ref=gathered.at[part, me],
            send_sem=gat_send.at[part, step], recv_sem=gat_recv.at[part, step],
            device_id={"replica": lax.rem(high + step, pairs) * 2 + low}, device_id_type=MESH,
        )

    def forward(part, step):
        origin = lax.rem(high + pairs - step, pairs) * 2 + low
        return pltpu.make_async_remote_copy(
            src_ref=gathered.at[part, origin], dst_ref=gathered.at[part, origin],
            send_sem=fwd_send.at[part, step], recv_sem=fwd_recv.at[part, step],
            device_id={"replica": partner}, device_id_type=MESH,
        )

    squares[me] = jnp.zeros((8, BLOCK), jnp.float32)

    def finish_part(part):
        @pl.loop(1, squares_count)
        def _(turn):
            sum_copy(part, turn).wait_recv()

        at_rows = rows_of(part)
        square = squares[me]
        for i in range(blocks_each):
            at = slice(i * BLOCK, (i + 1) * BLOCK)

            def add(turn, total):
                origin = lax.rem(my_square + squares_count - turn, squares_count)
                return total + unpack(arrived[origin, at_rows, at], most_square)

            total = lax.fori_loop(1, squares_count, add, own_sum[at_rows, at])
            gathered[part, me, :, at] = pack(total, most_all)
            value = total * spread[at_rows, span(place(me) + i * BLOCK, BLOCK)]
            square = square + jnp.sum((value * value).reshape(part_rows // 8, 8, BLOCK), axis=0)
        squares[me] = square

    def gather_part(part):
        forward(part, 0).start()

        @pl.loop(1, pairs)
        def _(step):
            gat_copy(part, step).start()

    def forward_part(part):
        @pl.loop(1, pairs)
        def _(step):
            gat_copy(part, step).wait_recv()
            forward(part, step).start()

    def sq_copy(step):
        return pltpu.make_async_remote_copy(
            src_ref=squares.at[me], dst_ref=squares.at[me],
            send_sem=sq_send.at[step], recv_sem=sq_recv.at[step],
            device_id={"replica": peer(step)}, device_id_type=MESH,
        )

    def ss_copy(step):
        return pltpu.make_async_remote_copy(
            src_ref=shard_squares.at[my_shard], dst_ref=shard_squares.at[my_shard],
            send_sem=ss_send.at[step], recv_sem=ss_recv.at[step],
            device_id={"shard": lax.rem(my_shard + step, shards)}, device_id_type=MESH,
        )

    for part in range(parts + 1):
        if part < parts:
            encode_part(part)
        if part >= 1:
            finish_part(part - 1)
            if part == parts:
                squares[me] = jnp.broadcast_to(jnp.sum(squares[me], axis=0, keepdims=True), (8, BLOCK))

                @pl.loop(1, workers)
                def _(step):
                    sq_copy(step).start()

            gather_part(part - 1)
        if part >= 2:
            forward_part(part - 2)

    for mate in range(3):
        top_copy(mate).wait()

    @pl.loop(0, SQUARE * quarter_blocks)
    def _(block):
        spread_column(block)

    def decode(part, worker):
        at = span(place(worker), width)
        gradient_out[rows_of(part), at] = unpack(gathered[part, worker], most_all) * spread[rows_of(part), at]

    for part in range(parts):
        @pl.loop(0, pairs)
        def _(step):
            origin = lax.rem(high + pairs - step, pairs) * 2 + low
            if part < parts - 1:
                decode(part, origin)

    forward_part(parts - 1)

    @pl.loop(1, workers)
    def _(step):
        sq_copy(step).wait()

    part_sum = squares[0]
    for w in range(1, workers):
        part_sum = part_sum + squares[w]
    shard_squares[my_shard] = part_sum

    @pl.loop(1, shards)
    def _(step):
        ss_copy(step).start()

    @pl.loop(0, pairs)
    def _(step):
        decode(parts - 1, lax.rem(high + pairs - step, pairs) * 2 + low)

    for part in range(parts):
        @pl.loop(0, pairs)
        def _(step):
            forward(part, step).wait_recv()
            decode(part, lax.rem(high + pairs - step, pairs) * 2 + 1 - low)

    @pl.loop(1, shards)
    def _(step):
        ss_copy(step).wait()

    part_sum = shard_squares[0]
    for s in range(1, shards):
        part_sum = part_sum + shard_squares[s]
    mean = jnp.sum(part_sum, axis=1, keepdims=True) / entry_count
    root_mean = jnp.sqrt(mean + epsilon)
    factor_out[...] = jnp.broadcast_to(jnp.minimum(1.0, clip_level / root_mean), factor_out.shape)

    @pl.loop(0, parts)
    def _(part):
        for mate in range(3):
            raw_copy(part, mate).wait_send()

        @pl.loop(1, squares_count)
        def _(turn):
            sum_copy(part, turn).wait_send()

        @pl.loop(1, pairs)
        def _(step):
            gat_copy(part, step).wait_send()

        @pl.loop(0, pairs)
        def _(step):
            forward(part, step).wait_send()

    momentum_copy.wait()


def exchange(outer_params, local_params, momentum):
    workers = lax.axis_size("replica")
    shards = lax.axis_size("shard")
    rows, cols = outer_params.shape
    blocks = cols // BLOCK
    width = cols // workers
    quarter = cols // SQUARE
    squares_count = workers // SQUARE
    pairs = workers // 2
    parts = PARTS
    dma = pltpu.SemaphoreType.DMA
    vmem = pl.BlockSpec(memory_space=pltpu.VMEM)
    hbm = pl.BlockSpec(memory_space=pltpu.HBM)
    anywhere = pl.BlockSpec(memory_space=pl.ANY)
    return pl.pallas_call(
        functools.partial(exchange_kernel, workers, shards, rows * shards * cols),
        out_shape=(
            jax.ShapeDtypeStruct((rows, cols), jnp.float32),
            jax.ShapeDtypeStruct((rows, cols), jnp.float32),
            jax.ShapeDtypeStruct((blocks, rows), jnp.float32),
            jax.ShapeDtypeStruct((8, BLOCK), jnp.float32),
        ),
        in_specs=[hbm, hbm, hbm],
        out_specs=(vmem, anywhere, vmem, vmem),
        scratch_shapes=[
            pltpu.VMEM((rows, cols), jnp.float32),
            pltpu.VMEM((rows, cols), jnp.bfloat16),
            pltpu.VMEM((3, rows, quarter), jnp.bfloat16),
            pltpu.VMEM((blocks, rows), jnp.float32),
            pltpu.VMEM((workers, blocks // SQUARE, rows), jnp.float32),
            pltpu.VMEM((rows, quarter), jnp.float32),
            pltpu.VMEM((rows, cols), jnp.float32),
            pltpu.VMEM((rows, width), jnp.float32),
            pltpu.VMEM((squares_count, rows, width), jnp.bfloat16),
            pltpu.VMEM((squares_count, rows, width), jnp.bfloat16),
            pltpu.VMEM((parts, workers, rows // parts, width), jnp.bfloat16),
            pltpu.VMEM((workers, 8, BLOCK), jnp.float32),
            pltpu.VMEM((shards, 8, BLOCK), jnp.float32),
            dma((2, SQUARE)),
            dma((parts, 3)), dma((parts, 3)),
            dma((workers,)), dma((workers,)),
            dma((3,)), dma((3,)),
            dma((parts, squares_count)), dma((parts, squares_count)),
            dma((workers,)), dma((workers,)),
            dma((shards,)), dma((shards,)),
            dma((parts, pairs)), dma((parts, pairs)),
            dma((parts, pairs)), dma((parts, pairs)),
            dma(()),
        ],
        compiler_params=pltpu.CompilerParams(
            collective_id=0, has_side_effects=True, vmem_limit_bytes=24 * 2**20
        ),
        cost_estimate=pl.CostEstimate(
            flops=50 * rows * cols, bytes_accessed=8 * rows * cols * 4, transcendentals=0
        ),
    )(*(pltpu.with_memory_space_constraint(x, pltpu.HBM) for x in (outer_params, local_params, momentum)))


def finish_kernel(
    factor_ref, outer_ref, gradient_ref, momentum_ref, max_ref, params_out, next_out, max_out,
    params_v, next_v, sem, max_sem,
):
    tiles = sem.shape[1]
    rows = outer_ref.shape[0] // tiles
    maxima = pltpu.make_async_copy(max_ref, max_out, max_sem)
    maxima.start()

    def stores(tile):
        at = pl.ds(tile * rows, rows)
        return (
            pltpu.make_async_copy(next_v.at[at], next_out.at[at], sem.at[0, tile]),
            pltpu.make_async_copy(params_v.at[at], params_out.at[at], sem.at[1, tile]),
        )

    factor = factor_ref[0:1, 0:1]

    @pl.loop(0, tiles)
    def _(tile):
        at = pl.ds(pl.multiple_of(tile * rows, rows), rows)
        clipped = factor * gradient_ref[at, :]
        momentum_next = outer_decay * momentum_ref[at, :] + clipped
        next_v[at, :] = momentum_next
        params_v[at, :] = outer_ref[at, :] - outer_rate * (clipped + outer_decay * momentum_next)
        for copy in stores(tile):
            copy.start()

    @pl.loop(0, tiles)
    def _(tile):
        for copy in stores(tile):
            copy.wait()

    maxima.wait()


def finish(factor, outer_params, gradient, momentum, absmax):
    rows, cols = outer_params.shape
    tiles = rows // 16
    vmem = pl.BlockSpec(memory_space=pltpu.VMEM)
    hbm = pl.BlockSpec(memory_space=pltpu.HBM)
    return pl.pallas_call(
        finish_kernel,
        out_shape=(
            pltpu.HBM((rows, cols), jnp.float32),
            pltpu.HBM((rows, cols), jnp.float32),
            pltpu.HBM(absmax.shape, jnp.float32),
        ),
        in_specs=[vmem] * 5,
        out_specs=(hbm, hbm, hbm),
        scratch_shapes=[
            pltpu.VMEM((rows, cols), jnp.float32),
            pltpu.VMEM((rows, cols), jnp.float32),
            pltpu.SemaphoreType.DMA((2, tiles)),
            pltpu.SemaphoreType.DMA(()),
        ],
        compiler_params=pltpu.CompilerParams(vmem_limit_bytes=16 * 2**20),
        cost_estimate=pl.CostEstimate(
            flops=6 * rows * cols, bytes_accessed=18 * rows * cols, transcendentals=0
        ),
    )(factor, outer_params, gradient, momentum, absmax)


def per_device(outer_params, local_params, momentum):
    gradient, momentum, absmax, factor = exchange(outer_params, local_params, momentum)
    return finish(factor, outer_params, gradient, momentum, absmax)


def solution(mesh):
    return jax.shard_map(
        per_device,
        mesh=mesh,
        in_specs=(P("shard", None), P("replica", "shard", None), P("shard", None)),
        out_specs=(P("shard", None), P("shard", None), P(None, "shard")),
        check_vma=False,
    )
```

```python
import functools

import jax
import jax.numpy as jnp
from jax import lax
from jax.experimental import pallas as pl
from jax.experimental.pallas import tpu as pltpu
from jax.sharding import PartitionSpec as P

BLOCK = 128
MESH = pl.DeviceIdType.MESH

epsilon = 1e-06
clip_level = 0.5
outer_rate = 0.7
outer_decay = 0.9
grid_levels = 7.0

SMOOTH = (6.57973588, -12.98785441, 12.20756634, -6.687892761, 2.368806331, -0.5120006377)
SHIFT = 1.5 * 2.0**23
SQUARE = 4
CODE_RANGE = 112.0
SPLIT = (1, 2, 2, 2, 1)
DIRECT = 1
PIECES = 8
AHEAD = 3
TURN = {"encode": 0.0, "quad": 2.2, "finish": 5.75, "pass": 6.8, "sent": 7.0, "decode": 7.1}
FILL = (1.6, 5.3, 5.35)


def smooth_rest(rest):
    square = rest * rest
    value = SMOOTH[-1]
    for coefficient in SMOOTH[-2::-1]:
        value = value * square + coefficient
    return rest * square * value


def column_of(row):
    return jnp.broadcast_to(row, (BLOCK, row.shape[1])).T


def encode(deltas, inverse):
    values = deltas * inverse
    nearest = (values + SHIFT) - SHIFT
    rest = smooth_rest(smooth_rest(values - nearest))
    return (nearest + rest).astype(jnp.bfloat16).astype(jnp.float32)


def pack(total, most):
    return jnp.exp2(total * (CODE_RANGE / most)).astype(jnp.bfloat16)


def unpack(code, most):
    return jnp.log2(code.astype(jnp.float32)) * (most / CODE_RANGE)


def exchange_kernel(
    workers, shards, entry_count,
    outer_hbm, local_hbm, momentum_hbm, outer_v, gradient_out, momentum_out, max_out, factor_out,
    local_v, raw, local_max, max_slots, inverse, spread, pair_own, pair_out, pair_in, quads,
    gathered, squares,
    load_sem, raw_send, raw_recv, max_send, max_recv, top_send, top_recv, pair_send, pair_recv,
    quad_send, quad_recv, line_send, line_recv, pass_send, pass_recv, sq_send, sq_recv, momentum_sem,
):
    me = lax.axis_index("replica")
    my_shard = lax.axis_index("shard")
    rows, cols = outer_v.shape
    quarter, eighth = cols // 4, cols // 8
    group_blocks = quarter // BLOCK
    half_blocks = eighth // BLOCK
    count = workers // SQUARE
    parts = len(SPLIT)
    starts = [rows * sum(SPLIT[:part]) // sum(SPLIT) for part in range(parts + 1)]
    most = [grid_levels * 2, grid_levels * SQUARE, grid_levels * workers]

    position = lax.rem(me, SQUARE)
    my_square = me // SQUARE
    low = lax.rem(position, 2)
    beside = position + 1 - 2 * low
    across = lax.rem(position + 2, SQUARE)
    diagonal = lax.rem(beside + 2, SQUARE)
    mates = (diagonal, beside, across)

    def pick(kind, first, second):
        return (first, second)[kind]

    def in_square(place):
        return {"replica": my_square * SQUARE + place}

    def first_mate(kind):
        return in_square(pick(kind, beside, across))

    def second_mate(kind):
        return in_square(pick(kind, across, beside))

    def group_of(kind, place):
        return kind * 2 + pick(kind, lax.rem(place, 2), place // 2)

    def half_of(kind, place):
        return pick(kind, place // 2, lax.rem(place, 2))

    def span(start, size):
        return pl.ds(pl.multiple_of(start, BLOCK), size)

    def rows_of(part):
        return slice(starts[part], starts[part + 1])

    def group_rows(group):
        return pl.ds(pl.multiple_of(group * group_blocks, group_blocks), group_blocks)

    def place_of(kind, place):
        return group_of(kind, place) * quarter + half_of(kind, place) * eighth

    def square_at(step):
        return lax.rem(my_square + step, count)

    def square_from(step):
        return lax.rem(my_square + count - step, count)

    def peer(step):
        return lax.rem(me + step, workers)

    def in_line(step):
        return {"replica": square_at(step) * SQUARE + position}

    def in_shard(step):
        return {"shard": lax.rem(my_shard + step, shards)}

    pieces = load_sem.shape[1]
    piece = cols // pieces

    def loads(i):
        part = pl.ds(i * piece, piece)
        return (
            pltpu.make_async_copy(outer_hbm.at[:, part], outer_v.at[:, part], load_sem.at[0, i]),
            pltpu.make_async_copy(local_hbm.at[0, :, part], local_v.at[:, part], load_sem.at[1, i]),
        )

    for i in range(pieces):
        for copy in loads(i):
            copy.start()

    barrier = pltpu.get_barrier_semaphore()
    for step in range(1, workers):
        pl.semaphore_signal(barrier, inc=1, device_id={"replica": peer(step)}, device_id_type=MESH)
    beyond = [in_shard(step) for step in range(1, shards)]
    beyond += [in_square(mate) | in_shard(step) for mate in mates for step in range(1, shards)]
    for device in beyond:
        pl.semaphore_signal(barrier, inc=1, device_id=device, device_id_type=MESH)

    def remote(source, target, send, recv, device):
        return pltpu.make_async_remote_copy(
            src_ref=source, dst_ref=target, send_sem=send, recv_sem=recv, device_id=device, device_id_type=MESH
        )

    def wait_bytes(ref, sem):
        pltpu.make_async_copy(ref, ref, sem).wait()

    def raw_copy(kind, part):
        other = (kind * 4 + 1 - group_of(kind, position)) * quarter
        return remote(
            local_v.at[rows_of(part), span(other, quarter)], raw.at[kind, rows_of(part)],
            raw_send, raw_recv.at[kind, part], first_mate(kind),
        )

    per_piece = piece // BLOCK
    for i in range(pieces):
        for copy in loads(i):
            copy.wait()

        for j in range(per_piece):
            block = i * per_piece + j
            at = slice(block * BLOCK, (block + 1) * BLOCK)
            deltas = outer_v[:, at] - local_v[:, at].astype(jnp.float32)
            local_max[block : block + 1, :] = jnp.max(jnp.abs(deltas).T, axis=0, keepdims=True)

    pl.semaphore_wait(barrier, workers - 1 + len(beyond))

    for step in range(workers - 1, 0, -1):
        for kind in range(2):
            remote(
                local_max.at[group_rows(group_of(kind, lax.rem(peer(step), SQUARE)))], max_slots.at[step, kind],
                max_send, max_recv, {"replica": peer(step)},
            ).start()

    def raw_start(part):
        for kind in range(2):
            raw_copy(kind, part).start()

    ahead = min(AHEAD, parts)
    for part in range(ahead):
        raw_start(part)

    momentum_copy = pltpu.make_async_copy(momentum_hbm, momentum_out, momentum_sem)
    momentum_copy.start()
    arrived = max_slots.at[pl.ds(1, workers - 1)]
    wait_bytes(arrived, max_recv)

    def top_copy(kind):
        at = group_rows(group_of(kind, position))
        return remote(max_out.at[at], max_out.at[at], top_send, top_recv, first_mate(kind))

    def invert(kind):
        absmax = local_max[group_rows(group_of(kind, position))]
        for step in range(1, workers):
            absmax = jnp.maximum(absmax, max_slots[step, kind])
        max_out[group_rows(group_of(kind, position))] = absmax
        quotient = grid_levels / (absmax + epsilon)
        for block in range(group_blocks):
            inverse[kind, :, block * BLOCK : (block + 1) * BLOCK] = column_of(quotient[block : block + 1, :])

    def top_start():
        for kind in range(2):
            top_copy(kind).start()

    def top_wait():
        wait_bytes(max_slots.at[0], top_recv)

    def spread_group(group):
        share = (max_out[group_rows(group)] + epsilon) * (1.0 / (grid_levels * workers))
        for block in range(group_blocks):
            spread[:, span(group * quarter + block * BLOCK, BLOCK)] = column_of(share[block : block + 1, :])

    def own_spread():
        for kind in range(2):
            spread_group(group_of(kind, position))

    def other_spread(kind):
        spread_group(kind * 4 + 1 - group_of(kind, position))

    def pair_sum(kind, part, block):
        at_rows = rows_of(part)
        at = span(group_of(kind, position) * quarter + block * BLOCK, BLOCK)
        here = span(block * BLOCK, BLOCK)
        outer = outer_v[at_rows, at]
        inv = inverse[kind, at_rows, here]
        return encode(outer - local_v[at_rows, at].astype(jnp.float32), inv) + encode(
            outer - raw[kind, at_rows, here].astype(jnp.float32), inv
        )

    def pair_copy(kind, part):
        return remote(
            pair_out.at[kind, rows_of(part)], pair_in.at[kind, rows_of(part)],
            pair_send, pair_recv.at[kind, part], second_mate(kind),
        )

    def encode_part(kind, part):
        raw_copy(kind, part).wait_recv()
        mine = half_of(kind, position)
        for i in range(half_blocks):
            pair_out[kind, rows_of(part), i * BLOCK : (i + 1) * BLOCK] = pack(
                pair_sum(kind, part, (1 - mine) * half_blocks + i), most[0]
            )
        for i in range(half_blocks):
            pair_own[kind, rows_of(part), i * BLOCK : (i + 1) * BLOCK] = pair_sum(
                kind, part, mine * half_blocks + i
            )
        pair_copy(kind, part).start()

    def quad_part(kind, part):
        pair_copy(kind, part).wait_recv()
        at = (kind, rows_of(part))
        quads[my_square, kind, rows_of(part)] = pack(pair_own[at] + unpack(pair_in[at], most[0]), most[1])
        for step in range(1, count):
            slot = quads.at[my_square, kind, rows_of(part)]
            remote(slot, slot, quad_send, quad_recv.at[part, step], in_line(step)).start()

    def line_copy(part):
        slot = gathered.at[position, :, rows_of(part)]
        return remote(slot, slot, line_send, line_recv.at[part], in_square(across))

    def direct(part):
        return part >= parts - DIRECT

    def pass_copy(part, side):
        alone = side == 1 and direct(part)
        slot = gathered.at[across if side == 1 and not alone else position, :, rows_of(part)]
        return remote(slot, slot, pass_send, pass_recv.at[part, side], in_square(diagonal if alone else beside))

    mine = my_shard * SQUARE + position
    squares[mine] = jnp.zeros((8, BLOCK), jnp.float32)

    def finish_part(part):
        for step in range(1, count):
            wait_bytes(quads.at[square_from(step), :, rows_of(part)], quad_recv.at[part, step])

        at_rows = rows_of(part)
        square = squares[mine]
        for kind in range(2):
            for i in range(half_blocks):
                at = slice(i * BLOCK, (i + 1) * BLOCK)
                total = unpack(quads[0, kind, at_rows, at], most[1])
                for other in range(1, count):
                    total = total + unpack(quads[other, kind, at_rows, at], most[1])
                gathered[position, kind, at_rows, at] = pack(total, most[2])
                value = total * spread[at_rows, span(place_of(kind, position) + i * BLOCK, BLOCK)]
                square = square + jnp.sum((value * value).reshape(-1, 8, BLOCK), axis=0)
        squares[mine] = square

    def gather_part(part):
        if direct(part):
            pass_copy(part, 1).start()
        line_copy(part).start()
        pass_copy(part, 0).start()

    def pass_part(part):
        line_copy(part).wait_recv()
        if not direct(part):
            pass_copy(part, 1).start()

    def decode(part, place):
        for kind in range(2):
            at = span(place_of(kind, place), eighth)
            gradient_out[rows_of(part), at] = unpack(gathered[place, kind, rows_of(part)], most[2]) * spread[rows_of(part), at]

    def decode_line(part):
        decode(part, position)
        decode(part, across)

    def decode_part(part):
        pass_copy(part, 0).wait_recv()
        decode(part, beside)
        pass_copy(part, 1).wait_recv()
        decode(part, diagonal)

    def squares_start():
        squares[mine] = jnp.broadcast_to(jnp.sum(squares[mine], axis=0, keepdims=True), (8, BLOCK))
        for device in [in_square(mate) for mate in mates] + beyond[::-1]:
            remote(squares.at[mine], squares.at[mine], sq_send, sq_recv, device).start()

    def sent_all():
        wait_bytes(raw, raw_send)
        wait_bytes(arrived, max_send)
        wait_bytes(max_slots.at[0], top_send)
        wait_bytes(pair_out, pair_send)
        wait_bytes(quads.at[pl.ds(0, count - 1)], quad_send)
        momentum_copy.wait()

    stages = []
    last = parts - 1
    for part in range(parts):
        for kind in range(2):
            stages.append((part + TURN["encode"] + 0.5 * kind, encode_part, (kind, part)))
            stages.append((part + TURN["quad"] + 0.5 * kind, quad_part, (kind, part)))
        if part + ahead < parts:
            stages.append((part + TURN["encode"] + 0.55, raw_start, (part + ahead,)))
        stages.append((part + TURN["finish"], finish_part, (part,)))
        if part == last:
            stages.append((part + TURN["finish"], squares_start, ()))
        stages.append((part + TURN["finish"], gather_part, (part,)))
        stages.append((part + TURN["pass"], pass_part, (part,)))
        stages.append((part * 0.01 + last + TURN["decode"], decode_line, (part,)))
        stages.append((part * 0.01 + last + TURN["decode"] + 0.05, decode_part, (part,)))
    for kind in range(2):
        stages.append((kind * 0.5 - 0.1, invert, (kind,)))
        stages.append((FILL[1 + kind], other_spread, (kind,)))
    stages.append((0.9, top_start, ()))
    stages.append((FILL[1] - 0.01, top_wait, ()))
    stages.append((FILL[0], own_spread, ()))
    stages.append((last + TURN["sent"], sent_all, ()))
    for _, stage, given in sorted(stages, key=lambda stage: stage[0]):
        stage(*given)

    others = squares.at[pl.ds(0, SQUARE * shards - 1)]
    wait_bytes(others, sq_recv)
    part_sum = squares[0]
    for slot in range(1, SQUARE * shards):
        part_sum = part_sum + squares[slot]
    mean = jnp.sum(part_sum, axis=1, keepdims=True) / entry_count
    root_mean = jnp.sqrt(mean + epsilon)
    factor_out[...] = jnp.broadcast_to(jnp.minimum(1.0, clip_level / root_mean), factor_out.shape)
    wait_bytes(others, sq_send)
    wait_bytes(gathered.at[0], line_send)
    wait_bytes(gathered.at[pl.ds(0, 2)], pass_send)


def exchange(outer_params, local_params, momentum):
    workers = lax.axis_size("replica")
    shards = lax.axis_size("shard")
    rows, cols = outer_params.shape
    blocks = cols // BLOCK
    quarter, eighth = cols // 4, cols // 8
    count = workers // SQUARE
    parts = len(SPLIT)
    dma = pltpu.SemaphoreType.DMA
    vmem = pl.BlockSpec(memory_space=pltpu.VMEM)
    hbm = pl.BlockSpec(memory_space=pltpu.HBM)
    anywhere = pl.BlockSpec(memory_space=pl.ANY)
    return pl.pallas_call(
        functools.partial(exchange_kernel, workers, shards, rows * shards * cols),
        out_shape=(
            jax.ShapeDtypeStruct((rows, cols), jnp.float32),
            jax.ShapeDtypeStruct((rows, cols), jnp.float32),
            jax.ShapeDtypeStruct((rows, cols), jnp.float32),
            jax.ShapeDtypeStruct((blocks, rows), jnp.float32),
            jax.ShapeDtypeStruct((8, BLOCK), jnp.float32),
        ),
        in_specs=[hbm, hbm, hbm],
        out_specs=(vmem, vmem, anywhere, vmem, vmem),
        scratch_shapes=[
            pltpu.VMEM((rows, cols), jnp.bfloat16),
            pltpu.VMEM((2, rows, quarter), jnp.bfloat16),
            pltpu.VMEM((blocks, rows), jnp.float32),
            pltpu.VMEM((workers, 2, blocks // 4, rows), jnp.float32),
            pltpu.VMEM((2, rows, quarter), jnp.float32),
            pltpu.VMEM((rows, cols), jnp.float32),
            pltpu.VMEM((2, rows, eighth), jnp.float32),
            pltpu.VMEM((2, rows, eighth), jnp.bfloat16),
            pltpu.VMEM((2, rows, eighth), jnp.bfloat16),
            pltpu.VMEM((count, 2, rows, eighth), jnp.bfloat16),
            pltpu.VMEM((SQUARE, 2, rows, eighth), jnp.bfloat16),
            pltpu.VMEM((SQUARE * shards, 8, BLOCK), jnp.float32),
            dma((2, PIECES)),
            dma(()), dma((2, parts)),
            dma(()), dma(()),
            dma(()), dma(()),
            dma(()), dma((2, parts)),
            dma(()), dma((parts, count)),
            dma(()), dma((parts,)),
            dma(()), dma((parts, 2)),
            dma(()), dma(()),
            dma(()),
        ],
        compiler_params=pltpu.CompilerParams(
            collective_id=0, has_side_effects=True, vmem_limit_bytes=24 * 2**20
        ),
        cost_estimate=pl.CostEstimate(
            flops=50 * rows * cols, bytes_accessed=8 * rows * cols * 4, transcendentals=0
        ),
    )(*(pltpu.with_memory_space_constraint(x, pltpu.HBM) for x in (outer_params, local_params, momentum)))


def finish_kernel(
    factor_ref, outer_ref, gradient_ref, momentum_ref, max_ref, params_out, next_out, max_out,
    params_v, next_v, sem, max_sem,
):
    tiles = sem.shape[1]
    rows = outer_ref.shape[0] // tiles
    maxima = pltpu.make_async_copy(max_ref, max_out, max_sem)
    maxima.start()

    def stores(tile):
        at = pl.ds(tile * rows, rows)
        return (
            pltpu.make_async_copy(next_v.at[at], next_out.at[at], sem.at[0, tile]),
            pltpu.make_async_copy(params_v.at[at], params_out.at[at], sem.at[1, tile]),
        )

    factor = factor_ref[0:1, 0:1]

    @pl.loop(0, tiles)
    def _(tile):
        at = pl.ds(pl.multiple_of(tile * rows, rows), rows)
        clipped = factor * gradient_ref[at, :]
        momentum_next = outer_decay * momentum_ref[at, :] + clipped
        next_v[at, :] = momentum_next
        params_v[at, :] = outer_ref[at, :] - outer_rate * (clipped + outer_decay * momentum_next)
        for copy in stores(tile):
            copy.start()

    @pl.loop(0, tiles)
    def _(tile):
        for copy in stores(tile):
            copy.wait()

    maxima.wait()


def finish(factor, outer_params, gradient, momentum, absmax):
    rows, cols = outer_params.shape
    tiles = rows // 16
    vmem = pl.BlockSpec(memory_space=pltpu.VMEM)
    hbm = pl.BlockSpec(memory_space=pltpu.HBM)
    return pl.pallas_call(
        finish_kernel,
        out_shape=(
            pltpu.HBM((rows, cols), jnp.float32),
            pltpu.HBM((rows, cols), jnp.float32),
            pltpu.HBM(absmax.shape, jnp.float32),
        ),
        in_specs=[vmem] * 5,
        out_specs=(hbm, hbm, hbm),
        scratch_shapes=[
            pltpu.VMEM((rows, cols), jnp.float32),
            pltpu.VMEM((rows, cols), jnp.float32),
            pltpu.SemaphoreType.DMA((2, tiles)),
            pltpu.SemaphoreType.DMA(()),
        ],
        compiler_params=pltpu.CompilerParams(vmem_limit_bytes=16 * 2**20),
        cost_estimate=pl.CostEstimate(
            flops=6 * rows * cols, bytes_accessed=18 * rows * cols, transcendentals=0
        ),
    )(factor, outer_params, gradient, momentum, absmax)


def per_device(outer_params, local_params, momentum):
    outer, gradient, momentum, absmax, factor = exchange(outer_params, local_params, momentum)
    return finish(factor, outer, gradient, momentum, absmax)


def solution(mesh):
    return jax.shard_map(
        per_device,
        mesh=mesh,
        in_specs=(P("shard", None), P("replica", "shard", None), P("shard", None)),
        out_specs=(P("shard", None), P("shard", None), P(None, "shard")),
        check_vma=False,
    )
```

```python
import functools

import jax
import jax.numpy as jnp
from jax import lax
from jax.experimental import pallas as pl
from jax.experimental.pallas import tpu as pltpu
from jax.sharding import PartitionSpec as P

BLOCK = 128
MESH = pl.DeviceIdType.MESH

epsilon = 1e-06
clip_level = 0.5
outer_rate = 0.7
outer_decay = 0.9
grid_levels = 7.0

SMOOTH = (6.57973588, -12.98785441, 12.20756634, -6.687892761, 2.368806331, -0.5120006377)
SHIFT = 1.5 * 2.0**23
SQUARE = 4
CODE_RANGE = 112.0
SPLIT = (1, 1, 2, 2, 1, 1)
DIRECT = 3
WHOLE = 0
EARLY = (4.1, 5.6, 0.7)
PIECES = 4
TILE = 16
LANES = 1
BEFORE = 8
HALF = 8
AHEAD = 3
TURN = {"encode": 0.0, "quad": 2.2, "finish": 4.75, "pass": 6.8, "sent": 7.0, "decode": 7.1}
FILL = (1.6, 5.3, 5.35)


def smooth_rest(rest):
    square = rest * rest
    value = SMOOTH[-1]
    for coefficient in SMOOTH[-2::-1]:
        value = value * square + coefficient
    return rest * square * value


def column_of(row):
    return jnp.broadcast_to(row, (BLOCK, row.shape[1])).T


def encode(deltas, inverse):
    values = deltas * inverse
    nearest = (values + SHIFT) - SHIFT
    rest = smooth_rest(smooth_rest(values - nearest))
    return (nearest + rest).astype(jnp.bfloat16).astype(jnp.float32)


def pack(total, most):
    return jnp.exp2(total * (CODE_RANGE / most)).astype(jnp.bfloat16)


def unpack(code, most):
    return jnp.log2(code.astype(jnp.float32)) * (most / CODE_RANGE)


def exchange_kernel(
    workers, shards, entry_count,
    outer_hbm, local_hbm, momentum_hbm, outer_v, gradient_out, momentum_out, max_out, factor_out,
    local_v, raw, raw_whole, local_max, packed_max, max_slots, inverse, spread, pair_own, pair_out, pair_in, quads,
    gathered, squares,
    load_sem, whole_send, whole_recv, raw_send, raw_recv, max_send, max_recv, top_send, top_recv, pair_send, pair_recv,
    quad_send, quad_recv, line_send, line_recv, pass_send, pass_recv, sq_send, sq_recv, momentum_sem,
):
    me = lax.axis_index("replica")
    my_shard = lax.axis_index("shard")
    rows, cols = outer_v.shape
    quarter, eighth = cols // 4, cols // 8
    group_blocks = quarter // BLOCK
    half_blocks = eighth // BLOCK
    count = workers // SQUARE
    parts = len(SPLIT)
    starts = [rows * sum(SPLIT[:part]) // sum(SPLIT) for part in range(parts + 1)]
    most = [grid_levels * 2, grid_levels * SQUARE, grid_levels * workers]

    position = lax.rem(me, SQUARE)
    my_square = me // SQUARE
    low = lax.rem(position, 2)
    beside = position + 1 - 2 * low
    across = lax.rem(position + 2, SQUARE)
    diagonal = lax.rem(beside + 2, SQUARE)
    mates = (diagonal, beside, across)

    def pick(kind, first, second):
        return (first, second)[kind]

    def in_square(place):
        return {"replica": my_square * SQUARE + place}

    def first_mate(kind):
        return in_square(pick(kind, beside, across))

    def second_mate(kind):
        return in_square(pick(kind, across, beside))

    def group_of(kind, place):
        return kind * 2 + pick(kind, place % 2 if isinstance(place, int) else lax.rem(place, 2), place // 2)

    def half_of(kind, place):
        return pick(kind, place // 2, lax.rem(place, 2))

    def span(start, size):
        return pl.ds(pl.multiple_of(start, BLOCK), size)

    def rows_of(part):
        return slice(starts[part], starts[part + 1])

    def group_rows(group):
        return pl.ds(group * group_blocks if isinstance(group, int) else pl.multiple_of(group * group_blocks, group_blocks), group_blocks)

    def place_of(kind, place):
        return group_of(kind, place) * quarter + half_of(kind, place) * eighth

    def square_at(step):
        return lax.rem(my_square + step, count)

    def square_from(step):
        return lax.rem(my_square + count - step, count)

    def peer(step):
        return lax.rem(me + step, workers)

    def in_line(step):
        return {"replica": square_at(step) * SQUARE + position}

    def in_shard(step):
        return {"shard": lax.rem(my_shard + step, shards)}

    pieces = load_sem.shape[1]
    piece = cols // pieces

    def loads(i):
        part = pl.ds(i * piece, piece)
        return (
            pltpu.make_async_copy(outer_hbm.at[:, part], outer_v.at[:, part], load_sem.at[0, i]),
            pltpu.make_async_copy(local_hbm.at[0, :, part], local_v.at[:, part], load_sem.at[1, i]),
        )

    for i in range(pieces):
        for copy in loads(i):
            copy.start()

    barrier = pltpu.get_barrier_semaphore()
    for step in range(1, workers):
        pl.semaphore_signal(barrier, inc=1, device_id={"replica": peer(step)}, device_id_type=MESH)
    beyond = [in_shard(step) for step in range(1, shards)]
    beyond += [in_square(mate) | in_shard(step) for mate in mates for step in range(1, shards)]
    for device in beyond:
        pl.semaphore_signal(barrier, inc=1, device_id=device, device_id_type=MESH)

    def remote(source, target, send, recv, device):
        return pltpu.make_async_remote_copy(
            src_ref=source, dst_ref=target, send_sem=send, recv_sem=recv, device_id=device, device_id_type=MESH
        )

    def wait_bytes(ref, sem):
        pltpu.make_async_copy(ref, ref, sem).wait()

    def raw_copy(kind, part):
        other = (kind * 4 + 1 - group_of(kind, position)) * quarter
        return remote(
            local_v.at[rows_of(part), span(other, quarter)], raw.at[kind, rows_of(part)],
            raw_send, raw_recv.at[kind, part], first_mate(kind),
        )

    def whole_copy(kind, part, mate):
        return remote(
            local_v.at[rows_of(part), span(place_of(kind, mates[mate]), eighth)], raw_whole.at[mate, kind, rows_of(part)],
            whole_send, whole_recv.at[part], in_square(mates[mate]),
        )

    per_piece = piece // BLOCK
    wide = lax.broadcasted_iota(jnp.int32, (rows, BLOCK), 1)

    def piece_lanes(i, found):
        for j in range(per_piece):
            block = i * per_piece + j
            at = slice(block * BLOCK, (block + 1) * BLOCK)
            deltas = outer_v[:, at] - local_v[:, at].astype(jnp.float32)
            found = jnp.where(wide == block, jnp.max(jnp.abs(deltas), axis=1, keepdims=True), found)
        return found

    def piece_max(i):
        for j in range(per_piece):
            block = i * per_piece + j
            at = slice(block * BLOCK, (block + 1) * BLOCK)
            deltas = outer_v[:, at] - local_v[:, at].astype(jnp.float32)
            local_max[block : block + 1, :] = jnp.max(jnp.abs(deltas).T, axis=0, keepdims=True)

    found = jnp.zeros((rows, BLOCK), jnp.float32)
    for i in range(pieces):
        for copy in loads(i):
            copy.wait()
        if LANES:
            found = piece_lanes(i, found)
        else:
            piece_max(i)
    if LANES:
        local_max[...] = found.T[: cols // BLOCK]

    for place in range(SQUARE):
        for kind in range(2):
            packed_max[place, kind] = local_max[group_rows(group_of(kind, place))]

    pl.semaphore_wait(barrier, workers - 1 + len(beyond))

    def max_send_to(step, place):
        slot = lax.rem(step * SQUARE + lax.rem(place + SQUARE - position, SQUARE), workers)
        remote(
            packed_max.at[place], max_slots.at[slot], max_send, max_recv,
            {"replica": square_at(step) * SQUARE + place},
        ).start()

    for step in range(count - 1, -1, -1):
        for place in (diagonal, across, beside, position):
            if step > 0 or place is not position:
                max_send_to(step, place)

    def whole(part):
        return part < WHOLE

    def raw_start(part):
        if whole(part):
            for mate in range(3):
                for kind in range(2):
                    whole_copy(kind, part, mate).start()
        else:
            for kind in range(2):
                raw_copy(kind, part).start()

    ahead = min(AHEAD, parts)
    for part in range(ahead):
        raw_start(part)

    momentum_copy = pltpu.make_async_copy(momentum_hbm, momentum_out, momentum_sem)
    momentum_copy.start()
    arrived = max_slots.at[pl.ds(1, workers - 1)]
    wait_bytes(arrived, max_recv)

    def top_copy(kind):
        at = group_rows(group_of(kind, position))
        return remote(max_out.at[at], max_out.at[at], top_send, top_recv, first_mate(kind))

    def invert(kind):
        absmax = local_max[group_rows(group_of(kind, position))]
        for step in range(1, workers):
            absmax = jnp.maximum(absmax, max_slots[step, kind])
        max_out[group_rows(group_of(kind, position))] = absmax
        quotient = grid_levels / (absmax + epsilon)
        for block in range(group_blocks):
            inverse[kind, :, block * BLOCK : (block + 1) * BLOCK] = column_of(quotient[block : block + 1, :])

    def top_start():
        for kind in range(2):
            top_copy(kind).start()

    def top_wait():
        wait_bytes(max_slots.at[0], top_recv)

    def spread_group(group):
        share = (max_out[group_rows(group)] + epsilon) * (1.0 / (grid_levels * workers))
        for block in range(group_blocks):
            spread[:, span(group * quarter + block * BLOCK, BLOCK)] = column_of(share[block : block + 1, :])

    def own_spread():
        for kind in range(2):
            spread_group(group_of(kind, position))

    def other_spread(kind):
        spread_group(kind * 4 + 1 - group_of(kind, position))

    def pair_sum(kind, part, block):
        at_rows = rows_of(part)
        at = span(group_of(kind, position) * quarter + block * BLOCK, BLOCK)
        here = span(block * BLOCK, BLOCK)
        outer = outer_v[at_rows, at]
        inv = inverse[kind, at_rows, here]
        return encode(outer - local_v[at_rows, at].astype(jnp.float32), inv) + encode(
            outer - raw[kind, at_rows, here].astype(jnp.float32), inv
        )

    def pair_copy(kind, part):
        return remote(
            pair_out.at[kind, rows_of(part)], pair_in.at[kind, rows_of(part)],
            pair_send, pair_recv.at[kind, part], second_mate(kind),
        )

    def whole_part(part):
        wait_bytes(raw_whole.at[:, :, rows_of(part)], whole_recv.at[part])
        for kind in range(2):
            mine = half_of(kind, position) * eighth
            for i in range(half_blocks):
                at_rows = rows_of(part)
                here = slice(i * BLOCK, (i + 1) * BLOCK)
                at = span(place_of(kind, position) + i * BLOCK, BLOCK)
                outer = outer_v[at_rows, at]
                inv = inverse[kind, at_rows, span(mine + i * BLOCK, BLOCK)]
                total = encode(outer - local_v[at_rows, at].astype(jnp.float32), inv)
                for mate in range(3):
                    total = total + encode(outer - raw_whole[mate, kind, at_rows, here].astype(jnp.float32), inv)
                quads[my_square, kind, at_rows, here] = pack(total, most[1])
            quad_start(kind, part)

    def quad_start(kind, part):
        for step in range(1, count):
            slot = quads.at[my_square, kind, rows_of(part)]
            remote(slot, slot, quad_send, quad_recv.at[part, step - 1], in_line(step)).start()

    def encode_part(kind, part):
        raw_copy(kind, part).wait_recv()
        mine = half_of(kind, position)
        for i in range(half_blocks):
            pair_out[kind, rows_of(part), i * BLOCK : (i + 1) * BLOCK] = pack(
                pair_sum(kind, part, (1 - mine) * half_blocks + i), most[0]
            )
        for i in range(half_blocks):
            pair_own[kind, rows_of(part), i * BLOCK : (i + 1) * BLOCK] = pair_sum(
                kind, part, mine * half_blocks + i
            )
        pair_copy(kind, part).start()

    def quad_part(kind, part):
        pair_copy(kind, part).wait_recv()
        at = (kind, rows_of(part))
        quads[my_square, kind, rows_of(part)] = pack(pair_own[at] + unpack(pair_in[at], most[0]), most[1])
        quad_start(kind, part)

    def line_copy(part):
        slot = gathered.at[position, :, rows_of(part)]
        return remote(slot, slot, line_send, line_recv.at[part], in_square(across))

    def direct(part):
        return part >= parts - DIRECT

    def pass_copy(part, side):
        alone = side == 1 and direct(part)
        slot = gathered.at[across if side == 1 and not alone else position, :, rows_of(part)]
        return remote(slot, slot, pass_send, pass_recv.at[part, side], in_square(diagonal if alone else beside))

    mine = my_shard * SQUARE + position
    squares[mine] = jnp.zeros((8, BLOCK), jnp.float32)

    def finish_part(part):
        for step in range(1, count):
            wait_bytes(quads.at[square_from(step), :, rows_of(part)], quad_recv.at[part, step - 1])

        at_rows = rows_of(part)
        square = squares[mine]
        for kind in range(2):
            for i in range(half_blocks):
                at = slice(i * BLOCK, (i + 1) * BLOCK)
                total = unpack(quads[0, kind, at_rows, at], most[1])
                for other in range(1, count):
                    total = total + unpack(quads[other, kind, at_rows, at], most[1])
                gathered[position, kind, at_rows, at] = pack(total, most[2])
                value = total * spread[at_rows, span(place_of(kind, position) + i * BLOCK, BLOCK)]
                square = square + jnp.sum((value * value).reshape(-1, 8, BLOCK), axis=0)
        squares[mine] = square

    def gather_part(part):
        if direct(part):
            pass_copy(part, 1).start()
        line_copy(part).start()
        pass_copy(part, 0).start()

    def pass_part(part):
        line_copy(part).wait_recv()
        if not direct(part):
            pass_copy(part, 1).start()

    def decode(part, place):
        for kind in range(2):
            at = span(place_of(kind, place), eighth)
            gradient_out[rows_of(part), at] = unpack(gathered[place, kind, rows_of(part)], most[2]) * spread[rows_of(part), at]

    def decode_line(part):
        decode(part, position)
        decode(part, across)

    def decode_part(part):
        pass_copy(part, 0).wait_recv()
        decode(part, beside)
        pass_copy(part, 1).wait_recv()
        decode(part, diagonal)

    def squares_start():
        squares[mine] = jnp.broadcast_to(jnp.sum(squares[mine], axis=0, keepdims=True), (8, BLOCK))
        for device in [in_square(mate) for mate in mates] + beyond[::-1]:
            remote(squares.at[mine], squares.at[mine], sq_send, sq_recv, device).start()

    def sent_all():
        split_rows = pl.ds(starts[WHOLE], rows - starts[WHOLE])
        whole_rows = pl.ds(0, starts[WHOLE])
        if WHOLE > 0:
            wait_bytes(raw_whole.at[:, :, whole_rows], whole_send)
        wait_bytes(raw.at[:, split_rows], raw_send)
        wait_bytes(arrived, max_send)
        wait_bytes(max_slots.at[0], top_send)
        wait_bytes(pair_out.at[:, split_rows], pair_send)
        wait_bytes(quads.at[pl.ds(0, count - 1)], quad_send)
        momentum_copy.wait()

    stages = []
    last = parts - 1
    for part in range(parts):
        if whole(part):
            stages.append((part * 0.1 + 0.45, whole_part, (part,)))
        for kind in range(0 if whole(part) else 2):
            stages.append((part + TURN["encode"] + 0.5 * kind, encode_part, (kind, part)))
            stages.append((part + TURN["quad"] + 0.5 * kind, quad_part, (kind, part)))
        if part + ahead < parts:
            stages.append((part + TURN["encode"] + 0.55, raw_start, (part + ahead,)))
        finish = EARLY[0] + part * EARLY[2] if whole(part) else part + TURN["finish"]
        stages.append((finish, finish_part, (part,)))
        if part == last:
            stages.append((finish, squares_start, ()))
        stages.append((finish, gather_part, (part,)))
        passing = EARLY[1] + part * EARLY[2] if whole(part) else part + TURN["pass"]
        stages.append((passing, pass_part, (part,)))
        stages.append((part * 0.01 + last + TURN["decode"], decode_line, (part,)))
        stages.append((part * 0.01 + last + TURN["decode"] + 0.05, decode_part, (part,)))
    for kind in range(2):
        stages.append((kind * 0.5 - 0.1, invert, (kind,)))
        stages.append((FILL[1 + kind], other_spread, (kind,)))
    stages.append((0.9, top_start, ()))
    stages.append((FILL[1] - 0.01, top_wait, ()))
    stages.append((FILL[0], own_spread, ()))
    stages.append((last + TURN["sent"], sent_all, ()))
    for _, stage, given in sorted(stages, key=lambda stage: stage[0]):
        stage(*given)

    others = squares.at[pl.ds(0, SQUARE * shards - 1)]
    wait_bytes(others, sq_recv)
    part_sum = squares[0]
    for slot in range(1, SQUARE * shards):
        part_sum = part_sum + squares[slot]
    mean = jnp.sum(part_sum, axis=1, keepdims=True) / entry_count
    root_mean = jnp.sqrt(mean + epsilon)
    factor_out[...] = jnp.broadcast_to(jnp.minimum(1.0, clip_level / root_mean), factor_out.shape)
    wait_bytes(others, sq_send)
    wait_bytes(gathered.at[0], line_send)
    wait_bytes(gathered.at[pl.ds(0, 2)], pass_send)


def exchange(outer_params, local_params, momentum):
    workers = lax.axis_size("replica")
    shards = lax.axis_size("shard")
    rows, cols = outer_params.shape
    blocks = cols // BLOCK
    quarter, eighth = cols // 4, cols // 8
    count = workers // SQUARE
    parts = len(SPLIT)
    dma = pltpu.SemaphoreType.DMA
    vmem = pl.BlockSpec(memory_space=pltpu.VMEM)
    hbm = pl.BlockSpec(memory_space=pltpu.HBM)
    anywhere = pl.BlockSpec(memory_space=pl.ANY)
    return pl.pallas_call(
        functools.partial(exchange_kernel, workers, shards, rows * shards * cols),
        out_shape=(
            jax.ShapeDtypeStruct((rows, cols), jnp.float32),
            jax.ShapeDtypeStruct((rows, cols), jnp.float32),
            jax.ShapeDtypeStruct((rows, cols), jnp.float32),
            jax.ShapeDtypeStruct((blocks, rows), jnp.float32),
            jax.ShapeDtypeStruct((8, BLOCK), jnp.float32),
        ),
        in_specs=[hbm, hbm, hbm],
        out_specs=(vmem, vmem, anywhere, vmem, vmem),
        scratch_shapes=[
            pltpu.VMEM((rows, cols), jnp.bfloat16),
            pltpu.VMEM((2, rows, quarter), jnp.bfloat16),
            pltpu.VMEM((3, 2, rows, eighth), jnp.bfloat16),
            pltpu.VMEM((blocks, rows), jnp.float32),
            pltpu.VMEM((SQUARE, 2, blocks // 4, rows), jnp.float32),
            pltpu.VMEM((workers, 2, blocks // 4, rows), jnp.float32),
            pltpu.VMEM((2, rows, quarter), jnp.float32),
            pltpu.VMEM((rows, cols), jnp.float32),
            pltpu.VMEM((2, rows, eighth), jnp.float32),
            pltpu.VMEM((2, rows, eighth), jnp.bfloat16),
            pltpu.VMEM((2, rows, eighth), jnp.bfloat16),
            pltpu.VMEM((count, 2, rows, eighth), jnp.bfloat16),
            pltpu.VMEM((SQUARE, 2, rows, eighth), jnp.bfloat16),
            pltpu.VMEM((SQUARE * shards, 8, BLOCK), jnp.float32),
            dma((2, PIECES)),
            dma(()), dma((max(WHOLE, 1),)),
            dma(()), dma((2, parts)),
            dma(()), dma(()),
            dma(()), dma(()),
            dma(()), dma((2, parts)),
            dma(()), dma((parts, count - 1)),
            dma(()), dma((parts,)),
            dma(()), dma((parts, 2)),
            dma(()), dma(()),
            dma(()),
        ],
        compiler_params=pltpu.CompilerParams(
            collective_id=0, has_side_effects=True, vmem_limit_bytes=24 * 2**20
        ),
        cost_estimate=pl.CostEstimate(
            flops=50 * rows * cols, bytes_accessed=8 * rows * cols * 4, transcendentals=0
        ),
    )(*(pltpu.with_memory_space_constraint(x, pltpu.HBM) for x in (outer_params, local_params, momentum)))


def finish_kernel(
    factor_ref, outer_ref, gradient_ref, momentum_ref, max_ref, params_out, next_out, max_out,
    params_v, next_v, sem, max_sem,
):
    tiles = sem.shape[1]
    rows = outer_ref.shape[0] // tiles
    maxima = pltpu.make_async_copy(max_ref, max_out, max_sem)
    maxima.start()

    def stores(tile):
        at = pl.ds(tile * rows, rows)
        return (
            pltpu.make_async_copy(next_v.at[at], next_out.at[at], sem.at[0, tile]),
            pltpu.make_async_copy(params_v.at[at], params_out.at[at], sem.at[1, tile]),
        )

    factor = factor_ref[0:1, 0:1]

    @pl.loop(0, tiles)
    def _(tile):
        at = pl.ds(pl.multiple_of(tile * rows, rows), rows)
        clipped = factor * gradient_ref[at, :]
        momentum_next = outer_decay * momentum_ref[at, :] + clipped
        next_v[at, :] = momentum_next
        params_v[at, :] = outer_ref[at, :] - outer_rate * (clipped + outer_decay * momentum_next)
        for copy in stores(tile):
            copy.start()

    @pl.loop(0, tiles)
    def _(tile):
        for copy in stores(tile):
            copy.wait()

    maxima.wait()


def finish(factor, outer_params, gradient, momentum, absmax):
    rows, cols = outer_params.shape
    tiles = rows // TILE
    vmem = pl.BlockSpec(memory_space=pltpu.VMEM)
    hbm = pl.BlockSpec(memory_space=pltpu.HBM)
    return pl.pallas_call(
        finish_kernel,
        out_shape=(
            pltpu.HBM((rows, cols), jnp.float32),
            pltpu.HBM((rows, cols), jnp.float32),
            pltpu.HBM(absmax.shape, jnp.float32),
        ),
        in_specs=[vmem] * 5,
        out_specs=(hbm, hbm, hbm),
        scratch_shapes=[
            pltpu.VMEM((rows, cols), jnp.float32),
            pltpu.VMEM((rows, cols), jnp.float32),
            pltpu.SemaphoreType.DMA((2, tiles)),
            pltpu.SemaphoreType.DMA(()),
        ],
        compiler_params=pltpu.CompilerParams(vmem_limit_bytes=16 * 2**20),
        cost_estimate=pl.CostEstimate(
            flops=6 * rows * cols, bytes_accessed=18 * rows * cols, transcendentals=0
        ),
    )(factor, outer_params, gradient, momentum, absmax)


def per_device(outer_params, local_params, momentum):
    outer, gradient, momentum, absmax, factor = exchange(outer_params, local_params, momentum)
    return finish(factor, outer, gradient, momentum, absmax)


def solution(mesh):
    return jax.shard_map(
        per_device,
        mesh=mesh,
        in_specs=(P("shard", None), P("replica", "shard", None), P("shard", None)),
        out_specs=(P("shard", None), P("shard", None), P(None, "shard")),
        check_vma=False,
    )
```

```python
import functools

import jax
import jax.numpy as jnp
from jax import lax
from jax.experimental import pallas as pl
from jax.experimental.pallas import tpu as pltpu
from jax.sharding import PartitionSpec as P

BLOCK = 128
MESH = pl.DeviceIdType.MESH

epsilon = 1e-06
clip_level = 0.5
outer_rate = 0.7
outer_decay = 0.9
grid_levels = 7.0

SMOOTH = (6.57973588, -12.98785441, 12.20756634, -6.687892761, 2.368806331, -0.5120006377)
SHIFT = 1.5 * 2.0**23
SQUARE = 4
CODE_RANGE = 112.0
SPLIT = (1, 1, 2, 2, 1, 1)
DIRECT = 3
HOLD = 1
NEXT = 0.95
PIECES = 4
TILE = 16
AHEAD = 3
TURN = {"encode": 0.0, "quad": 2.2, "finish": 4.75, "pass": 6.8, "sent": 7.0, "decode": 7.1}
FILL = (1.6, 5.3, 5.35)


def smooth_rest(rest):
    square = rest * rest
    value = SMOOTH[-1]
    for coefficient in SMOOTH[-2::-1]:
        value = value * square + coefficient
    return rest * square * value


def column_of(row):
    return jnp.broadcast_to(row, (BLOCK, row.shape[1])).T


def encode(deltas, inverse):
    values = deltas * inverse
    nearest = (values + SHIFT) - SHIFT
    rest = smooth_rest(smooth_rest(values - nearest))
    return (nearest + rest).astype(jnp.bfloat16).astype(jnp.float32)


def pack(total, most):
    return jnp.exp2(total * (CODE_RANGE / most)).astype(jnp.bfloat16)


def unpack(code, most):
    return jnp.log2(code.astype(jnp.float32)) * (most / CODE_RANGE)


def exchange_kernel(
    workers, shards, entry_count,
    outer_hbm, local_hbm, momentum_hbm, outer_v, gradient_out, momentum_out, max_out, factor_out,
    local_v, raw, local_max, packed_max, max_slots, inverse, spread, pair_own, pair_out, pair_in, quads,
    gathered, squares,
    load_sem, raw_send, raw_recv, max_send, max_recv, top_send, top_recv, pair_send, pair_recv,
    quad_send, quad_recv, line_send, line_recv, pass_send, pass_recv, sq_send, sq_recv, momentum_sem,
):
    me = lax.axis_index("replica")
    my_shard = lax.axis_index("shard")
    rows, cols = outer_v.shape
    quarter, eighth = cols // 4, cols // 8
    group_blocks = quarter // BLOCK
    half_blocks = eighth // BLOCK
    count = workers // SQUARE
    parts = len(SPLIT)
    starts = [rows * sum(SPLIT[:part]) // sum(SPLIT) for part in range(parts + 1)]
    most = [grid_levels * 2, grid_levels * SQUARE, grid_levels * workers]

    position = lax.rem(me, SQUARE)
    my_square = me // SQUARE
    low = lax.rem(position, 2)
    beside = position + 1 - 2 * low
    across = lax.rem(position + 2, SQUARE)
    diagonal = lax.rem(beside + 2, SQUARE)
    mates = (diagonal, beside, across)

    def pick(kind, first, second):
        return (first, second)[kind]

    def in_square(place):
        return {"replica": my_square * SQUARE + place}

    def first_mate(kind):
        return in_square(pick(kind, beside, across))

    def second_mate(kind):
        return in_square(pick(kind, across, beside))

    def group_of(kind, place):
        return kind * 2 + pick(kind, place % 2 if isinstance(place, int) else lax.rem(place, 2), place // 2)

    def half_of(kind, place):
        return pick(kind, place // 2, lax.rem(place, 2))

    def span(start, size):
        return pl.ds(pl.multiple_of(start, BLOCK), size)

    def rows_of(part):
        return slice(starts[part], starts[part + 1])

    def group_rows(group):
        return pl.ds(group * group_blocks if isinstance(group, int) else pl.multiple_of(group * group_blocks, group_blocks), group_blocks)

    def place_of(kind, place):
        return group_of(kind, place) * quarter + half_of(kind, place) * eighth

    def square_at(step):
        return lax.rem(my_square + step, count)

    def square_from(step):
        return lax.rem(my_square + count - step, count)

    def peer(step):
        return lax.rem(me + step, workers)

    def in_line(step):
        return {"replica": square_at(step) * SQUARE + position}

    def in_shard(step):
        return {"shard": lax.rem(my_shard + step, shards)}

    pieces = load_sem.shape[1]
    piece = cols // pieces

    def loads(i):
        part = pl.ds(i * piece, piece)
        return (
            pltpu.make_async_copy(outer_hbm.at[:, part], outer_v.at[:, part], load_sem.at[0, i]),
            pltpu.make_async_copy(local_hbm.at[0, :, part], local_v.at[:, part], load_sem.at[1, i]),
        )

    for i in range(pieces):
        for copy in loads(i):
            copy.start()

    barrier = pltpu.get_barrier_semaphore()
    for step in range(1, workers):
        pl.semaphore_signal(barrier, inc=1, device_id={"replica": peer(step)}, device_id_type=MESH)
    beyond = [in_shard(step) for step in range(1, shards)]
    beyond += [in_square(mate) | in_shard(step) for mate in mates for step in range(1, shards)]
    for device in beyond:
        pl.semaphore_signal(barrier, inc=1, device_id=device, device_id_type=MESH)

    def remote(source, target, send, recv, device):
        return pltpu.make_async_remote_copy(
            src_ref=source, dst_ref=target, send_sem=send, recv_sem=recv, device_id=device, device_id_type=MESH
        )

    def wait_bytes(ref, sem):
        pltpu.make_async_copy(ref, ref, sem).wait()

    def raw_copy(kind, part):
        other = (kind * 4 + 1 - group_of(kind, position)) * quarter
        return remote(
            local_v.at[rows_of(part), span(other, quarter)], raw.at[kind, rows_of(part)],
            raw_send, raw_recv.at[kind, part], first_mate(kind),
        )

    per_piece = piece // BLOCK
    wide = lax.broadcasted_iota(jnp.int32, (rows, BLOCK), 1)

    def piece_lanes(i, found):
        for j in range(per_piece):
            block = i * per_piece + j
            at = slice(block * BLOCK, (block + 1) * BLOCK)
            deltas = outer_v[:, at] - local_v[:, at].astype(jnp.float32)
            found = jnp.where(wide == block, jnp.max(jnp.abs(deltas), axis=1, keepdims=True), found)
        return found

    found = jnp.zeros((rows, BLOCK), jnp.float32)
    for i in range(pieces):
        for copy in loads(i):
            copy.wait()
        found = piece_lanes(i, found)
    local_max[...] = found.T[: cols // BLOCK]

    for place in range(SQUARE):
        for kind in range(2):
            packed_max[place, kind] = local_max[group_rows(group_of(kind, place))]

    pl.semaphore_wait(barrier, workers - 1 + len(beyond))

    def max_send_to(step, place):
        slot = lax.rem(step * SQUARE + lax.rem(place + SQUARE - position, SQUARE), workers)
        remote(
            packed_max.at[place], max_slots.at[slot], max_send, max_recv,
            {"replica": square_at(step) * SQUARE + place},
        ).start()

    for step in range(count - 1, -1, -1):
        for place in (diagonal, across, beside, position):
            if step > 0 or place is not position:
                max_send_to(step, place)

    def raw_start(part):
        for kind in range(2):
            raw_copy(kind, part).start()

    ahead = min(AHEAD, parts)
    for part in range(ahead):
        raw_start(part)

    momentum_copy = pltpu.make_async_copy(momentum_hbm, momentum_out, momentum_sem)
    momentum_copy.start()
    arrived = max_slots.at[pl.ds(1, workers - 1)]
    wait_bytes(arrived, max_recv)

    def top_copy(kind):
        at = group_rows(group_of(kind, position))
        return remote(max_out.at[at], max_out.at[at], top_send, top_recv, first_mate(kind))

    def invert(kind):
        absmax = local_max[group_rows(group_of(kind, position))]
        for step in range(1, workers):
            absmax = jnp.maximum(absmax, max_slots[step, kind])
        max_out[group_rows(group_of(kind, position))] = absmax
        quotient = grid_levels / (absmax + epsilon)
        for block in range(group_blocks):
            inverse[kind, :, block * BLOCK : (block + 1) * BLOCK] = column_of(quotient[block : block + 1, :])

    def top_start():
        for kind in range(2):
            top_copy(kind).start()

    def top_wait():
        wait_bytes(max_slots.at[0], top_recv)

    def spread_group(group):
        share = (max_out[group_rows(group)] + epsilon) * (1.0 / (grid_levels * workers))
        for block in range(group_blocks):
            spread[:, span(group * quarter + block * BLOCK, BLOCK)] = column_of(share[block : block + 1, :])

    def own_spread():
        for kind in range(2):
            spread_group(group_of(kind, position))

    def other_spread(kind):
        spread_group(kind * 4 + 1 - group_of(kind, position))

    def pair_sum(kind, part, block):
        at_rows = rows_of(part)
        at = span(group_of(kind, position) * quarter + block * BLOCK, BLOCK)
        here = span(block * BLOCK, BLOCK)
        outer = outer_v[at_rows, at]
        inv = inverse[kind, at_rows, here]
        return encode(outer - local_v[at_rows, at].astype(jnp.float32), inv) + encode(
            outer - raw[kind, at_rows, here].astype(jnp.float32), inv
        )

    def pair_copy(kind, part):
        return remote(
            pair_out.at[kind, rows_of(part)], pair_in.at[kind, rows_of(part)],
            pair_send, pair_recv.at[kind, part], second_mate(kind),
        )

    def quad_start(kind, part):
        for step in range(1, count):
            slot = quads.at[my_square, kind, rows_of(part)]
            remote(slot, slot, quad_send, quad_recv.at[part, step - 1], in_line(step)).start()

    def encode_part(kind, part):
        raw_copy(kind, part).wait_recv()
        mine = half_of(kind, position)
        for i in range(half_blocks):
            pair_out[kind, rows_of(part), i * BLOCK : (i + 1) * BLOCK] = pack(
                pair_sum(kind, part, (1 - mine) * half_blocks + i), most[0]
            )
        for i in range(half_blocks):
            pair_own[kind, rows_of(part), i * BLOCK : (i + 1) * BLOCK] = pair_sum(
                kind, part, mine * half_blocks + i
            )
        pair_copy(kind, part).start()

    def quad_part(kind, part):
        pair_copy(kind, part).wait_recv()
        at = (kind, rows_of(part))
        quads[my_square, kind, rows_of(part)] = pack(pair_own[at] + unpack(pair_in[at], most[0]), most[1])
        quad_start(kind, part)

    def line_copy(part):
        slot = gathered.at[position, :, rows_of(part)]
        return remote(slot, slot, line_send, line_recv.at[part], in_square(across))

    def direct(part):
        return part >= parts - DIRECT

    def pass_copy(part, side):
        alone = side == 1 and direct(part)
        slot = gathered.at[across if side == 1 and not alone else position, :, rows_of(part)]
        return remote(slot, slot, pass_send, pass_recv.at[part, side], in_square(diagonal if alone else beside))

    mine = my_shard * SQUARE + position
    squares[mine] = jnp.zeros((8, BLOCK), jnp.float32)

    def finish_part(part):
        for step in range(1, count):
            wait_bytes(quads.at[square_from(step), :, rows_of(part)], quad_recv.at[part, step - 1])

        at_rows = rows_of(part)
        square = squares[mine]
        for kind in range(2):
            for i in range(half_blocks):
                at = slice(i * BLOCK, (i + 1) * BLOCK)
                total = unpack(quads[0, kind, at_rows, at], most[1])
                for other in range(1, count):
                    total = total + unpack(quads[other, kind, at_rows, at], most[1])
                gathered[position, kind, at_rows, at] = pack(total, most[2])
                value = total * spread[at_rows, span(place_of(kind, position) + i * BLOCK, BLOCK)]
                square = square + jnp.sum((value * value).reshape(-1, 8, BLOCK), axis=0)
        squares[mine] = square

    def gather_part(part):
        if direct(part):
            pass_copy(part, 1).start()
        line_copy(part).start()
        pass_copy(part, 0).start()

    def pass_part(part):
        line_copy(part).wait_recv()
        if not direct(part):
            pass_copy(part, 1).start()

    def decode(part, place):
        for kind in range(2):
            at = span(place_of(kind, place), eighth)
            gradient_out[rows_of(part), at] = unpack(gathered[place, kind, rows_of(part)], most[2]) * spread[rows_of(part), at]

    def decode_line(part):
        decode(part, position)
        decode(part, across)

    def decode_part(part):
        pass_copy(part, 0).wait_recv()
        decode(part, beside)
        pass_copy(part, 1).wait_recv()
        decode(part, diagonal)

    def squares_start():
        squares[mine] = jnp.broadcast_to(jnp.sum(squares[mine], axis=0, keepdims=True), (8, BLOCK))
        for device in [in_square(mate) for mate in mates] + beyond[::-1]:
            remote(squares.at[mine], squares.at[mine], sq_send, sq_recv, device).start()

    def sent_all():
        wait_bytes(raw, raw_send)
        wait_bytes(arrived, max_send)
        wait_bytes(max_slots.at[0], top_send)
        wait_bytes(pair_out, pair_send)
        wait_bytes(quads.at[pl.ds(0, count - 1)], quad_send)
        momentum_copy.wait()

    stages = []
    last = parts - 1
    for part in range(parts):
        for kind in range(2):
            stages.append((part + TURN["encode"] + 0.5 * kind, encode_part, (kind, part)))
            stages.append((part + TURN["quad"] + 0.5 * kind, quad_part, (kind, part)))
        if part + ahead < parts:
            stages.append((part + TURN["encode"] + NEXT, raw_start, (part + ahead,)))
        finish = part + TURN["finish"]
        stages.append((finish, finish_part, (part,)))
        if part == last:
            stages.append((finish, squares_start, ()))
        held = max(finish, last + TURN["finish"] + 0.01) if part + HOLD >= last else finish
        stages.append((held, gather_part, (part,)))
        stages.append((part + TURN["pass"], pass_part, (part,)))
        stages.append((part * 0.01 + last + TURN["decode"], decode_line, (part,)))
        stages.append((part * 0.01 + last + TURN["decode"] + 0.05, decode_part, (part,)))
    for kind in range(2):
        stages.append((kind * 0.5 - 0.1, invert, (kind,)))
        stages.append((FILL[1 + kind], other_spread, (kind,)))
    stages.append((0.9, top_start, ()))
    stages.append((FILL[1] - 0.01, top_wait, ()))
    stages.append((FILL[0], own_spread, ()))
    stages.append((last + TURN["sent"], sent_all, ()))
    for _, stage, given in sorted(stages, key=lambda stage: stage[0]):
        stage(*given)

    others = squares.at[pl.ds(0, SQUARE * shards - 1)]
    wait_bytes(others, sq_recv)
    part_sum = squares[0]
    for slot in range(1, SQUARE * shards):
        part_sum = part_sum + squares[slot]
    mean = jnp.sum(part_sum, axis=1, keepdims=True) / entry_count
    root_mean = jnp.sqrt(mean + epsilon)
    factor_out[...] = jnp.broadcast_to(jnp.minimum(1.0, clip_level / root_mean), factor_out.shape)
    wait_bytes(others, sq_send)
    wait_bytes(gathered.at[0], line_send)
    wait_bytes(gathered.at[pl.ds(0, 2)], pass_send)


def exchange(outer_params, local_params, momentum):
    workers = lax.axis_size("replica")
    shards = lax.axis_size("shard")
    rows, cols = outer_params.shape
    blocks = cols // BLOCK
    quarter, eighth = cols // 4, cols // 8
    count = workers // SQUARE
    parts = len(SPLIT)
    dma = pltpu.SemaphoreType.DMA
    vmem = pl.BlockSpec(memory_space=pltpu.VMEM)
    hbm = pl.BlockSpec(memory_space=pltpu.HBM)
    anywhere = pl.BlockSpec(memory_space=pl.ANY)
    return pl.pallas_call(
        functools.partial(exchange_kernel, workers, shards, rows * shards * cols),
        out_shape=(
            jax.ShapeDtypeStruct((rows, cols), jnp.float32),
            jax.ShapeDtypeStruct((rows, cols), jnp.float32),
            jax.ShapeDtypeStruct((rows, cols), jnp.float32),
            jax.ShapeDtypeStruct((blocks, rows), jnp.float32),
            jax.ShapeDtypeStruct((8, BLOCK), jnp.float32),
        ),
        in_specs=[hbm, hbm, hbm],
        out_specs=(vmem, vmem, anywhere, vmem, vmem),
        scratch_shapes=[
            pltpu.VMEM((rows, cols), jnp.bfloat16),
            pltpu.VMEM((2, rows, quarter), jnp.bfloat16),
            pltpu.VMEM((blocks, rows), jnp.float32),
            pltpu.VMEM((SQUARE, 2, blocks // 4, rows), jnp.float32),
            pltpu.VMEM((workers, 2, blocks // 4, rows), jnp.float32),
            pltpu.VMEM((2, rows, quarter), jnp.float32),
            pltpu.VMEM((rows, cols), jnp.float32),
            pltpu.VMEM((2, rows, eighth), jnp.float32),
            pltpu.VMEM((2, rows, eighth), jnp.bfloat16),
            pltpu.VMEM((2, rows, eighth), jnp.bfloat16),
            pltpu.VMEM((count, 2, rows, eighth), jnp.bfloat16),
            pltpu.VMEM((SQUARE, 2, rows, eighth), jnp.bfloat16),
            pltpu.VMEM((SQUARE * shards, 8, BLOCK), jnp.float32),
            dma((2, PIECES)),
            dma(()), dma((2, parts)),
            dma(()), dma(()),
            dma(()), dma(()),
            dma(()), dma((2, parts)),
            dma(()), dma((parts, count - 1)),
            dma(()), dma((parts,)),
            dma(()), dma((parts, 2)),
            dma(()), dma(()),
            dma(()),
        ],
        compiler_params=pltpu.CompilerParams(
            collective_id=0, has_side_effects=True, vmem_limit_bytes=24 * 2**20
        ),
        cost_estimate=pl.CostEstimate(
            flops=50 * rows * cols, bytes_accessed=8 * rows * cols * 4, transcendentals=0
        ),
    )(*(pltpu.with_memory_space_constraint(x, pltpu.HBM) for x in (outer_params, local_params, momentum)))


def finish_kernel(
    factor_ref, outer_ref, gradient_ref, momentum_ref, max_ref, params_out, next_out, max_out,
    params_v, next_v, sem, max_sem,
):
    tiles = sem.shape[1]
    rows = outer_ref.shape[0] // tiles
    maxima = pltpu.make_async_copy(max_ref, max_out, max_sem)
    maxima.start()

    def stores(tile):
        at = pl.ds(tile * rows, rows)
        return (
            pltpu.make_async_copy(next_v.at[at], next_out.at[at], sem.at[0, tile]),
            pltpu.make_async_copy(params_v.at[at], params_out.at[at], sem.at[1, tile]),
        )

    factor = factor_ref[0:1, 0:1]

    @pl.loop(0, tiles)
    def _(tile):
        at = pl.ds(pl.multiple_of(tile * rows, rows), rows)
        clipped = factor * gradient_ref[at, :]
        momentum_next = outer_decay * momentum_ref[at, :] + clipped
        next_v[at, :] = momentum_next
        params_v[at, :] = outer_ref[at, :] - outer_rate * (clipped + outer_decay * momentum_next)
        for copy in stores(tile):
            copy.start()

    @pl.loop(0, tiles)
    def _(tile):
        for copy in stores(tile):
            copy.wait()

    maxima.wait()


def finish(factor, outer_params, gradient, momentum, absmax):
    rows, cols = outer_params.shape
    tiles = rows // TILE
    vmem = pl.BlockSpec(memory_space=pltpu.VMEM)
    hbm = pl.BlockSpec(memory_space=pltpu.HBM)
    return pl.pallas_call(
        finish_kernel,
        out_shape=(
            pltpu.HBM((rows, cols), jnp.float32),
            pltpu.HBM((rows, cols), jnp.float32),
            pltpu.HBM(absmax.shape, jnp.float32),
        ),
        in_specs=[vmem] * 5,
        out_specs=(hbm, hbm, hbm),
        scratch_shapes=[
            pltpu.VMEM((rows, cols), jnp.float32),
            pltpu.VMEM((rows, cols), jnp.float32),
            pltpu.SemaphoreType.DMA((2, tiles)),
            pltpu.SemaphoreType.DMA(()),
        ],
        compiler_params=pltpu.CompilerParams(vmem_limit_bytes=16 * 2**20),
        cost_estimate=pl.CostEstimate(
            flops=6 * rows * cols, bytes_accessed=18 * rows * cols, transcendentals=0
        ),
    )(factor, outer_params, gradient, momentum, absmax)


def per_device(outer_params, local_params, momentum):
    outer, gradient, momentum, absmax, factor = exchange(outer_params, local_params, momentum)
    return finish(factor, outer, gradient, momentum, absmax)


def solution(mesh):
    return jax.shard_map(
        per_device,
        mesh=mesh,
        in_specs=(P("shard", None), P("replica", "shard", None), P("shard", None)),
        out_specs=(P("shard", None), P("shard", None), P(None, "shard")),
        check_vma=False,
    )
```

```python
import functools

import jax
import jax.numpy as jnp
from jax import lax
from jax.experimental import pallas as pl
from jax.experimental.pallas import tpu as pltpu
from jax.sharding import PartitionSpec as P

BLOCK = 128
MESH = pl.DeviceIdType.MESH

epsilon = 1e-06
clip_level = 0.5
outer_rate = 0.7
outer_decay = 0.9
grid_levels = 7.0

SMOOTH = (6.57973588, -12.98785441, 12.20756634, -6.687892761, 2.368806331, -0.5120006377)
SHIFT = 1.5 * 2.0**23
SQUARE = 4
CODE_RANGE = 112.0
SPLIT = (1, 1, 2, 2, 1, 1)
DIRECT = 3
HOLD = 1
NEXT = 0.95
PIECES = 4
TILE = 16
AHEAD = 3
TURN = {"encode": 0.0, "quad": 2.2, "finish": 4.75, "pass": 7.1, "sent": 8.0, "decode": 8.1}
FILL = (1.6, 5.3, 5.35)


def smooth_rest(rest):
    square = rest * rest
    value = SMOOTH[-1]
    for coefficient in SMOOTH[-2::-1]:
        value = value * square + coefficient
    return rest * square * value


def column_of(row):
    return jnp.broadcast_to(row, (BLOCK, row.shape[1])).T


def encode(deltas, inverse):
    values = deltas * inverse
    nearest = (values + SHIFT) - SHIFT
    rest = smooth_rest(smooth_rest(values - nearest))
    return (nearest + rest).astype(jnp.bfloat16).astype(jnp.float32)


def pack(total, most):
    return jnp.exp2(total * (CODE_RANGE / most)).astype(jnp.bfloat16)


def unpack(code, most):
    return jnp.log2(code.astype(jnp.float32)) * (most / CODE_RANGE)


def exchange_kernel(
    workers, shards, entry_count,
    outer_hbm, local_hbm, momentum_hbm, outer_v, gradient_out, momentum_out, max_out, factor_out,
    local_v, raw, local_max, packed_max, max_slots, inverse, spread, pair_own, pair_out, pair_in, quads,
    gathered, squares,
    load_sem, raw_send, raw_recv, max_send, max_recv, top_send, top_recv, pair_send, pair_recv,
    quad_send, quad_recv, line_send, line_recv, pass_send, pass_recv, sq_send, sq_recv, momentum_sem,
):
    me = lax.axis_index("replica")
    my_shard = lax.axis_index("shard")
    rows, cols = outer_v.shape
    quarter, eighth = cols // 4, cols // 8
    group_blocks = quarter // BLOCK
    half_blocks = eighth // BLOCK
    count = workers // SQUARE
    parts = len(SPLIT)
    starts = [rows * sum(SPLIT[:part]) // sum(SPLIT) for part in range(parts + 1)]
    most = [grid_levels * 2, grid_levels * SQUARE, grid_levels * workers]

    position = lax.rem(me, SQUARE)
    my_square = me // SQUARE
    low = lax.rem(position, 2)
    beside = position + 1 - 2 * low
    across = lax.rem(position + 2, SQUARE)
    diagonal = lax.rem(beside + 2, SQUARE)
    mates = (diagonal, beside, across)

    def pick(kind, first, second):
        return (first, second)[kind]

    def in_square(place):
        return {"replica": my_square * SQUARE + place}

    def first_mate(kind):
        return in_square(pick(kind, beside, across))

    def second_mate(kind):
        return in_square(pick(kind, across, beside))

    def group_of(kind, place):
        return kind * 2 + pick(kind, place % 2 if isinstance(place, int) else lax.rem(place, 2), place // 2)

    def half_of(kind, place):
        return pick(kind, place // 2, lax.rem(place, 2))

    def span(start, size):
        return pl.ds(pl.multiple_of(start, BLOCK), size)

    def rows_of(part):
        return slice(starts[part], starts[part + 1])

    def group_rows(group):
        return pl.ds(group * group_blocks if isinstance(group, int) else pl.multiple_of(group * group_blocks, group_blocks), group_blocks)

    def place_of(kind, place):
        return group_of(kind, place) * quarter + half_of(kind, place) * eighth

    def square_at(step):
        return lax.rem(my_square + step, count)

    def square_from(step):
        return lax.rem(my_square + count - step, count)

    def peer(step):
        return lax.rem(me + step, workers)

    def in_line(step):
        return {"replica": square_at(step) * SQUARE + position}

    def in_shard(step):
        return {"shard": lax.rem(my_shard + step, shards)}

    pieces = load_sem.shape[1]
    piece = cols // pieces

    def loads(i):
        part = pl.ds(i * piece, piece)
        return (
            pltpu.make_async_copy(outer_hbm.at[:, part], outer_v.at[:, part], load_sem.at[0, i]),
            pltpu.make_async_copy(local_hbm.at[0, :, part], local_v.at[:, part], load_sem.at[1, i]),
        )

    for i in range(pieces):
        for copy in loads(i):
            copy.start()

    barrier = pltpu.get_barrier_semaphore()
    for step in range(1, workers):
        pl.semaphore_signal(barrier, inc=1, device_id={"replica": peer(step)}, device_id_type=MESH)
    beyond = [in_shard(step) for step in range(1, shards)]
    beyond += [in_square(mate) | in_shard(step) for mate in mates for step in range(1, shards)]
    for device in beyond:
        pl.semaphore_signal(barrier, inc=1, device_id=device, device_id_type=MESH)

    def remote(source, target, send, recv, device):
        return pltpu.make_async_remote_copy(
            src_ref=source, dst_ref=target, send_sem=send, recv_sem=recv, device_id=device, device_id_type=MESH
        )

    def wait_bytes(ref, sem):
        pltpu.make_async_copy(ref, ref, sem).wait()

    def raw_copy(kind, part):
        other = (kind * 4 + 1 - group_of(kind, position)) * quarter
        return remote(
            local_v.at[rows_of(part), span(other, quarter)], raw.at[kind, rows_of(part)],
            raw_send, raw_recv.at[kind, part], first_mate(kind),
        )

    per_piece = piece // BLOCK
    wide = lax.broadcasted_iota(jnp.int32, (rows, BLOCK), 1)

    def piece_lanes(i, found):
        for j in range(per_piece):
            block = i * per_piece + j
            at = slice(block * BLOCK, (block + 1) * BLOCK)
            deltas = outer_v[:, at] - local_v[:, at].astype(jnp.float32)
            found = jnp.where(wide == block, jnp.max(jnp.abs(deltas), axis=1, keepdims=True), found)
        return found

    found = jnp.zeros((rows, BLOCK), jnp.float32)
    for i in range(pieces):
        for copy in loads(i):
            copy.wait()
        found = piece_lanes(i, found)
    local_max[...] = found.T[: cols // BLOCK]

    for place in range(SQUARE):
        for kind in range(2):
            packed_max[place, kind] = local_max[group_rows(group_of(kind, place))]

    pl.semaphore_wait(barrier, workers - 1 + len(beyond))

    def max_send_to(step, place):
        slot = lax.rem(step * SQUARE + lax.rem(place + SQUARE - position, SQUARE), workers)
        remote(
            packed_max.at[place], max_slots.at[slot], max_send, max_recv,
            {"replica": square_at(step) * SQUARE + place},
        ).start()

    for step in range(count - 1, -1, -1):
        for place in (diagonal, across, beside, position):
            if step > 0 or place is not position:
                max_send_to(step, place)

    def raw_start(part):
        for kind in (1, 0):
            raw_copy(kind, part).start()

    ahead = min(AHEAD, parts)
    for part in range(ahead):
        raw_start(part)

    momentum_copy = pltpu.make_async_copy(momentum_hbm, momentum_out, momentum_sem)
    momentum_copy.start()
    arrived = max_slots.at[pl.ds(1, workers - 1)]
    wait_bytes(arrived, max_recv)

    def top_copy(kind):
        at = group_rows(group_of(kind, position))
        return remote(max_out.at[at], max_out.at[at], top_send, top_recv, first_mate(kind))

    def invert(kind):
        absmax = local_max[group_rows(group_of(kind, position))]
        for step in range(1, workers):
            absmax = jnp.maximum(absmax, max_slots[step, kind])
        max_out[group_rows(group_of(kind, position))] = absmax
        quotient = grid_levels / (absmax + epsilon)
        for block in range(group_blocks):
            inverse[kind, :, block * BLOCK : (block + 1) * BLOCK] = column_of(quotient[block : block + 1, :])

    def top_start():
        for kind in range(2):
            top_copy(kind).start()

    def top_wait():
        wait_bytes(max_slots.at[0], top_recv)

    def spread_group(group):
        share = (max_out[group_rows(group)] + epsilon) * (1.0 / (grid_levels * workers))
        for block in range(group_blocks):
            spread[:, span(group * quarter + block * BLOCK, BLOCK)] = column_of(share[block : block + 1, :])

    def own_spread():
        for kind in range(2):
            spread_group(group_of(kind, position))

    def other_spread(kind):
        spread_group(kind * 4 + 1 - group_of(kind, position))

    def pair_sum(kind, part, block):
        at_rows = rows_of(part)
        at = span(group_of(kind, position) * quarter + block * BLOCK, BLOCK)
        here = span(block * BLOCK, BLOCK)
        outer = outer_v[at_rows, at]
        inv = inverse[kind, at_rows, here]
        return encode(outer - local_v[at_rows, at].astype(jnp.float32), inv) + encode(
            outer - raw[kind, at_rows, here].astype(jnp.float32), inv
        )

    def pair_copy(kind, part):
        return remote(
            pair_out.at[kind, rows_of(part)], pair_in.at[kind, rows_of(part)],
            pair_send, pair_recv.at[kind, part], second_mate(kind),
        )

    def quad_start(kind, part):
        for step in range(1, count):
            slot = quads.at[my_square, kind, rows_of(part)]
            remote(slot, slot, quad_send, quad_recv.at[part, step - 1], in_line(step)).start()

    def encode_part(kind, part):
        raw_copy(kind, part).wait_recv()
        mine = half_of(kind, position)
        for i in range(half_blocks):
            pair_out[kind, rows_of(part), i * BLOCK : (i + 1) * BLOCK] = pack(
                pair_sum(kind, part, (1 - mine) * half_blocks + i), most[0]
            )
        for i in range(half_blocks):
            pair_own[kind, rows_of(part), i * BLOCK : (i + 1) * BLOCK] = pair_sum(
                kind, part, mine * half_blocks + i
            )
        pair_copy(kind, part).start()

    def quad_part(kind, part):
        pair_copy(kind, part).wait_recv()
        at = (kind, rows_of(part))
        quads[my_square, kind, rows_of(part)] = pack(pair_own[at] + unpack(pair_in[at], most[0]), most[1])
        quad_start(kind, part)

    def line_copy(part):
        slot = gathered.at[position, :, rows_of(part)]
        return remote(slot, slot, line_send, line_recv.at[part], in_square(across))

    def direct(part):
        return part >= parts - DIRECT

    def pass_copy(part, side):
        alone = side == 1 and direct(part)
        slot = gathered.at[across if side == 1 and not alone else position, :, rows_of(part)]
        return remote(slot, slot, pass_send, pass_recv.at[part, side], in_square(diagonal if alone else beside))

    mine = my_shard * SQUARE + position
    squares[mine] = jnp.zeros((8, BLOCK), jnp.float32)

    def finish_part(part):
        for step in range(1, count):
            wait_bytes(quads.at[square_from(step), :, rows_of(part)], quad_recv.at[part, step - 1])

        at_rows = rows_of(part)
        square = squares[mine]
        for kind in range(2):
            for i in range(half_blocks):
                at = slice(i * BLOCK, (i + 1) * BLOCK)
                total = unpack(quads[0, kind, at_rows, at], most[1])
                for other in range(1, count):
                    total = total + unpack(quads[other, kind, at_rows, at], most[1])
                gathered[position, kind, at_rows, at] = pack(total, most[2])
                value = total * spread[at_rows, span(place_of(kind, position) + i * BLOCK, BLOCK)]
                square = square + jnp.sum((value * value).reshape(-1, 8, BLOCK), axis=0)
        squares[mine] = square

    def gather_part(part):
        if direct(part):
            pass_copy(part, 1).start()
        line_copy(part).start()
        pass_copy(part, 0).start()

    def pass_part(part):
        line_copy(part).wait_recv()
        if not direct(part):
            pass_copy(part, 1).start()

    def decode(part, place):
        for kind in range(2):
            at = span(place_of(kind, place), eighth)
            gradient_out[rows_of(part), at] = unpack(gathered[place, kind, rows_of(part)], most[2]) * spread[rows_of(part), at]

    def decode_line(part):
        decode(part, position)
        decode(part, across)

    def decode_part(part):
        pass_copy(part, 0).wait_recv()
        decode(part, beside)
        pass_copy(part, 1).wait_recv()
        decode(part, diagonal)

    def squares_start():
        squares[mine] = jnp.broadcast_to(jnp.sum(squares[mine], axis=0, keepdims=True), (8, BLOCK))
        for device in [in_square(mate) for mate in mates] + beyond[::-1]:
            remote(squares.at[mine], squares.at[mine], sq_send, sq_recv, device).start()

    def sent_all():
        wait_bytes(raw, raw_send)
        wait_bytes(arrived, max_send)
        wait_bytes(max_slots.at[0], top_send)
        wait_bytes(pair_out, pair_send)
        wait_bytes(quads.at[pl.ds(0, count - 1)], quad_send)
        momentum_copy.wait()

    stages = []
    last = parts - 1
    for part in range(parts):
        for kind in range(2):
            stages.append((part + TURN["encode"] + 0.5 * kind, encode_part, (kind, part)))
            stages.append((part + TURN["quad"] + 0.5 * kind, quad_part, (kind, part)))
        if part + ahead < parts:
            stages.append((part + TURN["encode"] + NEXT, raw_start, (part + ahead,)))
        finish = part + TURN["finish"]
        stages.append((finish, finish_part, (part,)))
        if part == last:
            stages.append((finish, squares_start, ()))
        held = max(finish, last + TURN["finish"] + 0.01) if part + HOLD >= last else finish
        stages.append((held, gather_part, (part,)))
        stages.append((part + TURN["pass"], pass_part, (part,)))
        stages.append((part * 0.01 + last + TURN["decode"], decode_line, (part,)))
        stages.append((part * 0.01 + last + TURN["decode"] + 0.05, decode_part, (part,)))
    for kind in range(2):
        stages.append((kind * 0.5 - 0.1, invert, (kind,)))
        stages.append((FILL[1 + kind], other_spread, (kind,)))
    stages.append((0.9, top_start, ()))
    stages.append((FILL[1] - 0.01, top_wait, ()))
    stages.append((FILL[0], own_spread, ()))
    stages.append((last + TURN["sent"], sent_all, ()))
    for _, stage, given in sorted(stages, key=lambda stage: stage[0]):
        stage(*given)

    others = squares.at[pl.ds(0, SQUARE * shards - 1)]
    wait_bytes(others, sq_recv)
    part_sum = squares[0]
    for slot in range(1, SQUARE * shards):
        part_sum = part_sum + squares[slot]
    mean = jnp.sum(part_sum, axis=1, keepdims=True) / entry_count
    root_mean = jnp.sqrt(mean + epsilon)
    factor_out[...] = jnp.broadcast_to(jnp.minimum(1.0, clip_level / root_mean), factor_out.shape)
    wait_bytes(others, sq_send)
    wait_bytes(gathered.at[0], line_send)
    wait_bytes(gathered.at[pl.ds(0, 2)], pass_send)


def exchange(outer_params, local_params, momentum):
    workers = lax.axis_size("replica")
    shards = lax.axis_size("shard")
    rows, cols = outer_params.shape
    blocks = cols // BLOCK
    quarter, eighth = cols // 4, cols // 8
    count = workers // SQUARE
    parts = len(SPLIT)
    dma = pltpu.SemaphoreType.DMA
    vmem = pl.BlockSpec(memory_space=pltpu.VMEM)
    hbm = pl.BlockSpec(memory_space=pltpu.HBM)
    anywhere = pl.BlockSpec(memory_space=pl.ANY)
    return pl.pallas_call(
        functools.partial(exchange_kernel, workers, shards, rows * shards * cols),
        out_shape=(
            jax.ShapeDtypeStruct((rows, cols), jnp.float32),
            jax.ShapeDtypeStruct((rows, cols), jnp.float32),
            jax.ShapeDtypeStruct((rows, cols), jnp.float32),
            jax.ShapeDtypeStruct((blocks, rows), jnp.float32),
            jax.ShapeDtypeStruct((8, BLOCK), jnp.float32),
        ),
        in_specs=[hbm, hbm, hbm],
        out_specs=(vmem, vmem, anywhere, vmem, vmem),
        scratch_shapes=[
            pltpu.VMEM((rows, cols), jnp.bfloat16),
            pltpu.VMEM((2, rows, quarter), jnp.bfloat16),
            pltpu.VMEM((blocks, rows), jnp.float32),
            pltpu.VMEM((SQUARE, 2, blocks // 4, rows), jnp.float32),
            pltpu.VMEM((workers, 2, blocks // 4, rows), jnp.float32),
            pltpu.VMEM((2, rows, quarter), jnp.float32),
            pltpu.VMEM((rows, cols), jnp.float32),
            pltpu.VMEM((2, rows, eighth), jnp.float32),
            pltpu.VMEM((2, rows, eighth), jnp.bfloat16),
            pltpu.VMEM((2, rows, eighth), jnp.bfloat16),
            pltpu.VMEM((count, 2, rows, eighth), jnp.bfloat16),
            pltpu.VMEM((SQUARE, 2, rows, eighth), jnp.bfloat16),
            pltpu.VMEM((SQUARE * shards, 8, BLOCK), jnp.float32),
            dma((2, PIECES)),
            dma(()), dma((2, parts)),
            dma(()), dma(()),
            dma(()), dma(()),
            dma(()), dma((2, parts)),
            dma(()), dma((parts, count - 1)),
            dma(()), dma((parts,)),
            dma(()), dma((parts, 2)),
            dma(()), dma(()),
            dma(()),
        ],
        compiler_params=pltpu.CompilerParams(
            collective_id=0, has_side_effects=True, vmem_limit_bytes=24 * 2**20
        ),
        cost_estimate=pl.CostEstimate(
            flops=50 * rows * cols, bytes_accessed=8 * rows * cols * 4, transcendentals=0
        ),
    )(*(pltpu.with_memory_space_constraint(x, pltpu.HBM) for x in (outer_params, local_params, momentum)))


def finish_kernel(
    factor_ref, outer_ref, gradient_ref, momentum_ref, max_ref, params_out, next_out, max_out,
    params_v, next_v, sem, max_sem,
):
    tiles = sem.shape[1]
    rows = outer_ref.shape[0] // tiles
    maxima = pltpu.make_async_copy(max_ref, max_out, max_sem)
    maxima.start()

    def stores(tile):
        at = pl.ds(tile * rows, rows)
        return (
            pltpu.make_async_copy(next_v.at[at], next_out.at[at], sem.at[0, tile]),
            pltpu.make_async_copy(params_v.at[at], params_out.at[at], sem.at[1, tile]),
        )

    factor = factor_ref[0:1, 0:1]

    @pl.loop(0, tiles)
    def _(tile):
        at = pl.ds(pl.multiple_of(tile * rows, rows), rows)
        clipped = factor * gradient_ref[at, :]
        momentum_next = outer_decay * momentum_ref[at, :] + clipped
        next_v[at, :] = momentum_next
        params_v[at, :] = outer_ref[at, :] - outer_rate * (clipped + outer_decay * momentum_next)
        for copy in stores(tile):
            copy.start()

    @pl.loop(0, tiles)
    def _(tile):
        for copy in stores(tile):
            copy.wait()

    maxima.wait()


def finish(factor, outer_params, gradient, momentum, absmax):
    rows, cols = outer_params.shape
    tiles = rows // TILE
    vmem = pl.BlockSpec(memory_space=pltpu.VMEM)
    hbm = pl.BlockSpec(memory_space=pltpu.HBM)
    return pl.pallas_call(
        finish_kernel,
        out_shape=(
            pltpu.HBM((rows, cols), jnp.float32),
            pltpu.HBM((rows, cols), jnp.float32),
            pltpu.HBM(absmax.shape, jnp.float32),
        ),
        in_specs=[vmem] * 5,
        out_specs=(hbm, hbm, hbm),
        scratch_shapes=[
            pltpu.VMEM((rows, cols), jnp.float32),
            pltpu.VMEM((rows, cols), jnp.float32),
            pltpu.SemaphoreType.DMA((2, tiles)),
            pltpu.SemaphoreType.DMA(()),
        ],
        compiler_params=pltpu.CompilerParams(vmem_limit_bytes=16 * 2**20),
        cost_estimate=pl.CostEstimate(
            flops=6 * rows * cols, bytes_accessed=18 * rows * cols, transcendentals=0
        ),
    )(factor, outer_params, gradient, momentum, absmax)


def per_device(outer_params, local_params, momentum):
    outer, gradient, momentum, absmax, factor = exchange(outer_params, local_params, momentum)
    return finish(factor, outer, gradient, momentum, absmax)


def solution(mesh):
    return jax.shard_map(
        per_device,
        mesh=mesh,
        in_specs=(P("shard", None), P("replica", "shard", None), P("shard", None)),
        out_specs=(P("shard", None), P("shard", None), P(None, "shard")),
        check_vma=False,
    )
```
